32 devices in a mesh: grp: 2 (over y), row: 16 (over z, x, core).
Axes of the slice: x: 2, y: 2, z: 4, core: 2. Of those that a mesh axis runs over, the one named last changes fastest.
Arguments:
- queries: bfloat16 [4096, 4096], P(('grp', 'row')), parts along dimension 0, may hold values from -130 to 130
- answer_keys: bfloat16 [4096, 512], P(('grp', 'row')), parts along dimension 0, may hold values from -6 to 6
- answer_values: bfloat16 [4096, 512], P(('grp', 'row')), parts along dimension 0, may hold values from -6 to 6
- prompt_keys: bfloat16 [256, 512], P(('grp', 'row')), parts along dimension 0, may hold values from -4 to 4
- prompt_values: bfloat16 [256, 512], P(('grp', 'row')), parts along dimension 0, may hold values from -6 to 6
- out_grad: bfloat16 [4096, 4096], P(('grp', 'row')), parts along dimension 0, may hold values from -6 to 6
- weights: float32 [4096], P(('grp', 'row')), parts along dimension 0, may hold values from 0.25 to 4
- lengths: int32 [64], P('grp'), parts along dimension 0, may hold values from 1 to 256, as said below
Outputs:
- attn_out: bfloat16 [4096, 4096], P(('grp', 'row')), parts along dimension 0
- q_grad: bfloat16 [4096, 4096], P(('grp', 'row')), parts along dimension 0
- answer_key_grad: bfloat16 [4096, 512], P(('grp', 'row')), parts along dimension 0
- answer_value_grad: bfloat16 [4096, 512], P(('grp', 'row')), parts along dimension 0
- prompt_key_grad: float32 [256, 512], P(('grp', 'row')), parts along dimension 0
- prompt_value_grad: float32 [256, 512], P(('grp', 'row')), parts along dimension 0
The draws below stay inside these ranges and needn't reach their ends.
There are 2 independent parts, one for each index of `grp`. The reference program is written for one: setup_inputs(seed, part) draws one part's arguments, and reference() takes and returns one part's arrays. A program takes and returns all parts, laid end to end along the dimension named above; each array names one. Nothing has to cross between parts.
Inputs may be any that keep to these rules, and one draw needn't show every extreme that they name: `lengths`: the answers fill the 2048 packed rows in order; the longest has exactly 256 rows.
All inputs are finite; a program needn't handle non-finite values.
Results may differ from the reference program's by a relative error of at most 0.02.
Values may be sent and summed in bfloat16 or wider, within the bound.
A program may use at most 192 MiB of HBM per device.

```python
import math
import jax
import jax.numpy as jnp
from jax import lax

HEADS = 32
KV_HEADS = 4
HEAD_DIM = 128
ROWS_DEV = 128
ROWS = 2048
PROMPT = 128
ANSWERS = 32
MOST_LEN = 256
N_ROW = 16


def drawn_pair(key):
    folded = jax.random.fold_in(key, 11)
    key_draw, query_draw = jax.random.split(folded, 2)
    prompt_rows = jnp.clip(jax.random.normal(key_draw, (PROMPT, KV_HEADS * HEAD_DIM), jnp.float32), -4.0, 4.0)
    queries = jnp.clip(3.0 * jax.random.normal(query_draw, (ROWS, HEADS * HEAD_DIM), jnp.float32), -18.0, 18.0)
    return (queries, prompt_rows)


def draw_queries(key, part):
    return drawn_pair(key)[0].astype(jnp.bfloat16)


def draw_prompt_keys(key, part):
    return drawn_pair(key)[1].astype(jnp.bfloat16)


def draw_lengths(key, part):
    total = ROWS - MOST_LEN - 1
    count = ANSWERS - 2
    height = MOST_LEN // 2
    spots = jnp.arange(1, total, dtype=jnp.int32)
    order = jax.random.permutation(jax.random.fold_in(key, 23), total - 1).astype(jnp.int32)
    inside = spots % height
    ranking = jnp.where(inside == height // 2, -1, jnp.where(inside == 0, total + order, order))
    picked = jnp.argsort(ranking, stable=True)[:count - 1]
    cuts = jnp.sort(spots[picked])
    edges = jnp.concatenate([jnp.zeros((1,), jnp.int32), cuts, jnp.full((1,), total, jnp.int32)])
    leading = edges[1:] - edges[:-1]
    closing = jnp.array([MOST_LEN, 1], dtype=jnp.int32)
    return jnp.concatenate([leading, closing]).astype(jnp.int32)


def block_levels(rng, dims, shards, least, largest):
    factor_of, own = 1.0, jax.random.fold_in(rng, 6)
    for axis_at, shards_of in shards:
        steps = jnp.exp(jax.random.uniform(jax.random.fold_in(own, axis_at), (shards_of,), jnp.float32, least / len(shards), largest / len(shards)))
        factor_of = factor_of * jnp.repeat(steps, dims[axis_at] // shards_of).reshape([-1 if axis == axis_at else 1 for axis in range(len(dims))])
    return factor_of


def scatter_about(key, extent, scale, bound, pieces=(), held_as=jnp.bfloat16):
    loudness = block_levels(key, extent, pieces, -0.22, 0.18) if pieces else 1.0
    values = jax.random.normal(key, extent, jnp.float32) * scale * loudness
    return jnp.minimum(jnp.maximum(values, -bound), bound).astype(held_as)


def setup_inputs(seed: int = 0, part: int = 0) -> dict:
    seeds = jax.random.split(jax.random.key(seed), 9)
    part_splits = jax.random.split(jax.random.fold_in(seeds[8], part), 9)
    return {
        "queries": draw_queries(jax.random.fold_in(jax.random.fold_in(seeds[8], part), 71), part),
        "answer_keys": scatter_about(part_splits[1], (ROWS, KV_HEADS * HEAD_DIM), 1.0, 6.0, ((0, 16),)),
        "answer_values": scatter_about(part_splits[2], (ROWS, KV_HEADS * HEAD_DIM), 1.0, 6.0, ((0, 16),)),
        "prompt_keys": draw_prompt_keys(jax.random.fold_in(jax.random.fold_in(seeds[8], part), 71), part),
        "prompt_values": scatter_about(part_splits[4], (PROMPT, KV_HEADS * HEAD_DIM), 1.0, 6.0, ((0, 16),)),
        "out_grad": scatter_about(part_splits[5], (ROWS, HEADS * HEAD_DIM), 1.0, 6.0, ((0, 16),)),
        "weights": jnp.clip(jnp.exp(math.log(4.0) - 2.7725887 * jax.random.uniform(part_splits[6], (ROWS,), jnp.float32) ** block_levels(part_splits[6], (ROWS,), ((0, 16),), -0.2, 0.2)), 0.25, 4.0),
        "lengths": draw_lengths(jax.random.fold_in(jax.random.fold_in(seeds[8], part), 71), part),
    }


MASKED = -1.0e30


def times_transposed(former, latter):
    return lax.dot_general(former, latter, (((1,), (1,)), ((), ())), preferred_element_type=jnp.float32)


def transposed_times(former, latter):
    return lax.dot_general(former, latter, (((0,), (0,)), ((), ())), preferred_element_type=jnp.float32)


def segment_of(positions, lengths):
    finish = jnp.cumsum(lengths, dtype=jnp.int32)
    starts = finish - lengths
    covered = (starts[None, :] <= positions[:, None]).astype(jnp.int32)
    return jnp.sum(covered, axis=1, dtype=jnp.int32) - 1


def probabilities(flat_queries, key_rows, allowed, group_size):
    key_count = key_rows.shape[0]
    height = allowed.shape[0]
    factor = key_rows.shape[1] ** -0.5
    scores = (times_transposed(flat_queries, key_rows) * factor).reshape(height, group_size, key_count)
    window = jnp.concatenate([jnp.ones((height, key_count - allowed.shape[1]), dtype=jnp.bool_), allowed], axis=1)
    scores = jnp.where(window[:, None, :], scores, MASKED)
    highest = jnp.max(scores, axis=2, keepdims=True)
    powers = jnp.exp(scores - highest)
    totals = jnp.sum(powers, axis=2, keepdims=True)
    return (powers / totals).reshape(height * group_size, key_count)


def block_terms(q_block, cot_block, key_rows, value_rows, allowed):
    height = q_block.shape[0]
    group_size = HEADS // KV_HEADS
    span_cols = group_size * HEAD_DIM
    factor = HEAD_DIM ** -0.5
    outputs, q_grads, key_terms, value_terms = [], [], [], []
    for kv_index in range(KV_HEADS):
        flat_queries = q_block[:, kv_index * span_cols:(kv_index + 1) * span_cols].reshape(height * group_size, HEAD_DIM)
        flat_cot = cot_block[:, kv_index * span_cols:(kv_index + 1) * span_cols].reshape(height * group_size, HEAD_DIM)
        key_slice = key_rows[:, kv_index * HEAD_DIM:(kv_index + 1) * HEAD_DIM]
        value_slice = value_rows[:, kv_index * HEAD_DIM:(kv_index + 1) * HEAD_DIM]
        chances = probabilities(flat_queries, key_slice, allowed, group_size)
        rounded = chances.astype(jnp.bfloat16)
        attended = jnp.dot(rounded, value_slice, preferred_element_type=jnp.float32).astype(jnp.bfloat16)
        row_delta = jnp.sum(flat_cot.astype(jnp.float32) * attended.astype(jnp.float32), axis=1, keepdims=True)
        slopes = times_transposed(flat_cot, value_slice)
        score_grad = (chances * (slopes - row_delta)).astype(jnp.bfloat16)
        q_part = (jnp.dot(score_grad, key_slice, preferred_element_type=jnp.float32) * factor).astype(jnp.bfloat16)
        outputs.append(attended.reshape(height, span_cols))
        q_grads.append(q_part.reshape(height, span_cols))
        key_terms.append(transposed_times(score_grad, flat_queries) * factor)
        value_terms.append(transposed_times(rounded, flat_cot))
    return (jnp.concatenate(outputs, axis=1), jnp.concatenate(q_grads, axis=1),
            jnp.concatenate(key_terms, axis=1), jnp.concatenate(value_terms, axis=1))


def reference(queries, answer_keys, answer_values, prompt_keys, prompt_values, out_grad, weights, lengths):
    height = ROWS_DEV
    columns = KV_HEADS * HEAD_DIM
    cotangent = (weights[:, None] * out_grad.astype(jnp.float32)).astype(jnp.bfloat16)
    padding = jnp.zeros((2 * height, columns), jnp.bfloat16)
    padded_keys = jnp.concatenate([padding, answer_keys], axis=0)
    padded_values = jnp.concatenate([padding, answer_values], axis=0)
    own_offsets = jnp.arange(height, dtype=jnp.int32)
    key_offsets = jnp.arange(3 * height, dtype=jnp.int32)

    def advance(running, block_index):
        prompt_key_sum, prompt_value_sum, answer_key_sum, answer_value_sum = running
        start_row = block_index * height
        q_block = lax.dynamic_slice_in_dim(queries, start_row, height, 0)
        cot_block = lax.dynamic_slice_in_dim(cotangent, start_row, height, 0)
        window_keys = lax.dynamic_slice_in_dim(padded_keys, start_row, 3 * height, 0)
        window_values = lax.dynamic_slice_in_dim(padded_values, start_row, 3 * height, 0)
        own_pos = start_row + own_offsets
        key_pos = start_row - 2 * height + key_offsets
        own_seg = segment_of(own_pos, lengths)
        key_seg = segment_of(key_pos, lengths)
        allowed = (key_pos[None, :] >= 0) & (key_pos[None, :] <= own_pos[:, None]) & (key_seg[None, :] == own_seg[:, None])
        key_rows = jnp.concatenate([prompt_keys, window_keys], axis=0)
        value_rows = jnp.concatenate([prompt_values, window_values], axis=0)
        outputs, q_grads, key_terms, value_terms = block_terms(q_block, cot_block, key_rows, value_rows, allowed)
        prompt_key_sum = prompt_key_sum + key_terms[:PROMPT]
        prompt_value_sum = prompt_value_sum + value_terms[:PROMPT]
        answer_key_sum = lax.dynamic_update_slice_in_dim(
            answer_key_sum, lax.dynamic_slice_in_dim(answer_key_sum, start_row, 3 * height, 0) + key_terms[PROMPT:], start_row, 0)
        answer_value_sum = lax.dynamic_update_slice_in_dim(
            answer_value_sum, lax.dynamic_slice_in_dim(answer_value_sum, start_row, 3 * height, 0) + value_terms[PROMPT:], start_row, 0)
        return (prompt_key_sum, prompt_value_sum, answer_key_sum, answer_value_sum), (outputs, q_grads)

    initial = (jnp.zeros((PROMPT, columns), jnp.float32), jnp.zeros((PROMPT, columns), jnp.float32),
               jnp.zeros((ROWS + 2 * height, columns), jnp.float32), jnp.zeros((ROWS + 2 * height, columns), jnp.float32))
    running, stacked = lax.scan(advance, initial, jnp.arange(N_ROW, dtype=jnp.int32))
    attn_out = stacked[0].reshape(ROWS, HEADS * HEAD_DIM)
    q_grad = stacked[1].reshape(ROWS, HEADS * HEAD_DIM)
    answer_key_grad = running[2][2 * height:].astype(jnp.bfloat16)
    answer_value_grad = running[3][2 * height:].astype(jnp.bfloat16)
    return attn_out, q_grad, answer_key_grad, answer_value_grad, running[0], running[1]
```

```python
import functools
import math

import jax
import jax.numpy as jnp
from jax import lax
from jax.experimental import pallas as pl
from jax.experimental.pallas import tpu as pltpu
from jax.sharding import PartitionSpec as P

HEAD_DIM = 128
MASKED = -1e30
MESH = pl.DeviceIdType.MESH


def dot(a, b):
    return jnp.dot(a, b, preferred_element_type=jnp.float32)


def twice(x):
    return jnp.concatenate([x, x], axis=1)


def kernel(
    n, kv_heads, group,
    q_hbm, og_hbm, ak, av, pk, pv, w, lens,
    attn, dq, akg, avg, pkg, pvg,
    qog, kall, vt, kt, pgath, wst, lst, qs_t, cots, cots_t, p_all, ds_all, acc,
    psend, precv, gsend, grecv, srecv, bias, tri_b,
    small_sem, in_sem, kv_sem, xq_recv, xk_recv, win_recv, pg_recv, pr_recv, gr_recv, sr_recv, at_recv, dq_recv,
    xs_send, xq_send, xk_send, win_send, pg_send, pr_send, gs_send, sr_send, at_send, dq_send, w_recv, w_send,
):
    me = lax.axis_index("row")
    height = ak.shape[0]
    d = HEAD_DIM
    span = group * d
    half = kv_heads // 2
    own_prompt = pk.shape[0]
    prompt = own_prompt * n
    factor = d ** (-0.5)
    log_factor = factor * math.log2(math.e)
    chips = n // 2
    core = lax.rem(me, 2)
    other = 1 - core
    chip = me // 2
    sibling = me + 1 - 2 * core
    after = lax.rem(chip + 1, chips)
    before = lax.rem(chip + chips - 1, chips)
    at1, at2, at3 = prompt, prompt + height, prompt + 2 * height

    def remote(src, dst, send, recv, target):
        return pltpu.make_async_remote_copy(
            src_ref=src, dst_ref=dst, send_sem=send, recv_sem=recv,
            device_id={"row": target}, device_id_type=MESH,
        )

    def cols(at, width):
        return pl.ds(pl.multiple_of(at * width, width), width)

    def block(b):
        return pl.ds(pl.multiple_of(prompt + b * height, height), height)

    def in_copies(j):
        head = core * half + j
        return (
            pltpu.make_async_copy(q_hbm.at[:, cols(head, span)], qog.at[1, j, 0], in_sem.at[j]),
            pltpu.make_async_copy(og_hbm.at[:, cols(head, span)], qog.at[1, j, 1], in_sem.at[j]),
        )

    def cross_copies(j):
        head = other * half + j
        return (
            remote(og_hbm.at[:, cols(head, span)], qog.at[0, j, 1], xq_send.at[j], xq_recv.at[j], sibling),
            remote(q_hbm.at[:, cols(head, span)], qog.at[0, j, 0], xq_send.at[j], xq_recv.at[j], sibling),
        )

    def kv_copies(j):
        head = core * half + j
        return [
            pltpu.make_async_copy(src.at[:, cols(head, d)], kall.at[j, i, block(2 + core)], kv_sem.at[j])
            for i, src in enumerate((ak, av))
        ]

    def kv_cross(j):
        head = other * half + j
        return [
            remote(src.at[:, cols(head, d)], kall.at[j, i, block(2 + core)], xk_send.at[j], xk_recv.at[j], sibling)
            for i, src in enumerate((ak, av))
        ]

    def win_copies(j):
        return [
            remote(
                src.at[:, pl.ds((t * half + j) * d, d)], kall.at[j, i, block(core)],
                win_send.at[j], win_recv.at[j], 2 * after + t,
            )
            for i, src in enumerate((ak, av)) for t in range(2)
        ]

    def prompt_copy(k, i):
        target = lax.rem(me + k, n)
        return remote(
            (pk, pv)[i].at[:, cols(lax.rem(target, 2), half * d)], pgath.at[i, me],
            pg_send, pg_recv, target,
        )

    def reduce_copy(j, k):
        target = lax.rem(me + k, n)
        return remote(psend.at[j, target], precv.at[core, j, chip], pr_send.at[j], pr_recv.at[j], target)

    def back_copy(j, t):
        return remote(gsend.at[j, t], grecv.at[core, j], gs_send.at[j], gr_recv.at[j], 2 * before + t)

    def sibling_copy(j):
        return remote(acc.at[j, :, block(2 + other)], srecv.at[j], sr_send.at[j], sr_recv.at[j], sibling)

    def out_copy(ref, j, send, recv):
        return remote(ref.at[0, j], ref.at[2, j], send.at[j], recv.at[j], sibling)

    barrier = pltpu.get_barrier_semaphore()

    @pl.loop(1, n)
    def _(k):
        pl.semaphore_signal(barrier, inc=1, device_id={"row": lax.rem(me + k, n)}, device_id_type=MESH)

    w_local = pltpu.make_async_copy(w, wst.at[1], small_sem.at[0])
    lens_local = pltpu.make_async_copy(lens, lst, small_sem.at[1])
    own_prompts = [
        pltpu.make_async_copy((pk, pv)[i].at[:, cols(core, half * d)], pgath.at[i, me], pg_recv) for i in range(2)
    ]
    w_local.start()
    lens_local.start()
    for j in range(half):
        for copy in in_copies(j):
            copy.start()
    for j in range(half):
        for copy in kv_copies(j):
            copy.start()
    for copy in own_prompts:
        copy.start()
    pl.semaphore_wait(barrier, n - 1)

    @pl.loop(1, n)
    def _(k):
        for i in range(2):
            prompt_copy(k, i).start()

    w_cross = remote(w, wst.at[0], w_send, w_recv, sibling)
    w_cross.start()
    for j in range(half):
        for copy in win_copies(j):
            copy.start()
        for copy in cross_copies(j):
            copy.start()
        for copy in kv_cross(j):
            copy.start()

    acc[...] = jnp.zeros(acc.shape, jnp.float32)
    lens_local.wait()
    answers = lens.shape[1]
    row = lax.broadcasted_iota(jnp.int32, (answers, answers), 0)
    col = lax.broadcasted_iota(jnp.int32, (answers, answers), 1)
    starts = jnp.sum(
        jnp.where(col < row, jnp.broadcast_to(lst[...], (answers, answers)), 0),
        axis=1, keepdims=True,
    )
    key = lax.broadcasted_iota(jnp.int32, (height, height), 0)
    query = lax.broadcasted_iota(jnp.int32, (height, height), 1)
    tri = key <= query
    for b in range(2):
        base = (2 * chip + b) * height
        pos = base + lax.broadcasted_iota(jnp.int32, (1, height), 1)
        first = jnp.max(jnp.where(starts <= pos, starts, 0), axis=0, keepdims=True)
        bias[b, 0] = jnp.where(key + (base - height) >= first, 0.0, MASKED)
        both = jnp.where(tri, key + base, key + (base - 2 * height))
        bias[b, 1] = jnp.where(both >= first, 0.0, MASKED)
    tri_b[...] = tri.astype(jnp.float32).astype(jnp.bfloat16)

    def prepare(s, j):
        for h in range(group):
            rows = slice(h * height, (h + 1) * height)
            og_t = qog[s, j, 1, :, rows].T
            cots_t[s, j, :, rows] = (wst[s] * og_t.astype(jnp.float32)).astype(jnp.bfloat16)
            qs_t[s, j, :, rows] = qog[s, j, 0, :, rows].T

    w_local.wait()

    @pl.loop(0, half)
    def _(j):
        pltpu.make_async_copy(qog.at[1, j], qog.at[1, j], in_sem.at[j]).wait()
        prepare(1, j)

    w_cross.wait_recv()

    @pl.loop(0, half)
    def _(j):
        pltpu.make_async_copy(qog.at[0, j], qog.at[0, j], xq_recv.at[j]).wait()
        prepare(0, j)

    pltpu.make_async_copy(pgath, pgath, pg_recv).wait()

    @pl.loop(0, 2 * half)
    def _(u):
        j = u // 2
        s = lax.rem(u, 2)
        b = s * core + (1 - s) * other

        @pl.when(s == 0)
        def _():
            mine = kall.at[j, :, block(2 + core)]
            pltpu.make_async_copy(mine, mine, kv_sem.at[j]).wait()
            theirs = kall.at[j, :, block(2 + other)]
            pltpu.make_async_copy(theirs, theirs, xk_recv.at[j]).wait()
            window = kall.at[j, :, pl.ds(prompt, 2 * height)]
            pltpu.make_async_copy(window, window, win_recv.at[j]).wait()
            for i in range(2):
                gathered = pgath[i, :, :, cols(j, d)].astype(jnp.float32).reshape(prompt, d)
                kall[j, i, :prompt, :] = gathered.astype(jnp.bfloat16)

        near_far = pl.ds(pl.multiple_of(prompt + b * height, height), 3 * height)
        tri2 = twice(tri)
        keys = jnp.concatenate([kall[j, 0, :prompt], kall[j, 0, near_far]], axis=0)
        values = jnp.concatenate([kall[j, 1, :prompt], kall[j, 1, near_far]], axis=0)
        vt[...] = values.T
        for pair in range(group // 2):
            rows = slice(pair * 2 * height, (pair + 1) * 2 * height)
            scores = dot(keys, qs_t[s, j, :, rows])
            s_p = scores[:at1]
            s_n = scores[at2:at3] + twice(bias[b, 0])
            s_c = jnp.where(tri2, scores[at3:], scores[at1:at2]) + twice(bias[b, 1])
            top = jnp.maximum(
                jnp.maximum(jnp.max(s_p, axis=0, keepdims=True), jnp.max(s_n, axis=0, keepdims=True)),
                jnp.max(s_c, axis=0, keepdims=True),
            )
            e_p = jnp.exp2((s_p - top) * log_factor)
            e_n = jnp.exp2((s_n - top) * log_factor)
            e_c = jnp.exp2((s_c - top) * log_factor)
            total = (
                jnp.sum(e_p, axis=0, keepdims=True)
                + jnp.sum(e_n, axis=0, keepdims=True)
                + jnp.sum(e_c, axis=0, keepdims=True)
            )
            inv = 1.0 / total
            p_all[s, j, :at1, rows] = e_p.astype(jnp.bfloat16)
            p_all[s, j, at2:at3, rows] = e_n.astype(jnp.bfloat16)
            b_c = e_c.astype(jnp.bfloat16)
            b_d = b_c * twice(tri_b[...])
            p_all[s, j, at1:at2, rows] = b_c - b_d
            p_all[s, j, at3:, rows] = b_d
            out_t = (dot(vt[...], p_all[s, j, :, rows]) * inv).astype(jnp.bfloat16)
            cot_t = (cots_t[s, j, :, rows].astype(jnp.float32) * inv).astype(jnp.bfloat16)
            delta = jnp.sum(
                cot_t.astype(jnp.float32) * out_t.astype(jnp.float32), axis=0, keepdims=True
            )
            slopes = dot(values, cot_t)
            ds_all[s, j, :, rows] = (
                p_all[s, j, :, rows].astype(jnp.float32) * (slopes - delta)
            ).astype(jnp.bfloat16)
            cots[rows, :] = cot_t.T
            out = out_t.T
            for h in range(2):
                lanes = slice((2 * pair + h) * d, (2 * pair + h + 1) * d)
                attn[s, j, :, lanes] = out[h * height : (h + 1) * height]

        q_rows = jnp.concatenate([qog[s, j, 0, :, h * d : (h + 1) * d] for h in range(group)], axis=0)
        for i in range(2):
            part = dot(ds_all[s, j], q_rows) * factor if i == 0 else dot(p_all[s, j], cots[...])
            acc[j, i, :prompt] += part[:at1]
            acc[j, i, near_far] += part[at1:]

        @pl.when(s == 0)
        def _():
            out_copy(attn, j, at_send, at_recv).start()

        @pl.when(s == 1)
        def _():
            for i in range(2):
                psend[j, :, i] = acc[j, i, :prompt].reshape(n, own_prompt, d).astype(jnp.bfloat16)
                for t in range(2):
                    gsend[j, t, i] = acc[j, i, prompt + t * height : prompt + (t + 1) * height].astype(jnp.bfloat16)

            @pl.loop(1, n)
            def _(k):
                reduce_copy(j, k).start()

            pltpu.make_async_copy(psend.at[j, me], precv.at[core, j, chip], pr_recv.at[j]).start()
            for t in range(2):
                back_copy(j, t).start()
            sibling_copy(j).start()

    @pl.loop(0, 2 * half)
    def _(u):
        s = u // half
        j = lax.rem(u, half)
        b = s * core + (1 - s) * other
        near_far = pl.ds(pl.multiple_of(prompt + b * height, height), 3 * height)
        kt[:, :at1] = kall[j, 0, :prompt].T
        kt[:, at1:] = kall[j, 0, near_far].T
        dq_t = (dot(kt[...], ds_all[s, j]) * factor).astype(jnp.bfloat16)
        for h in range(group):
            rows = slice(h * height, (h + 1) * height)
            dq[s, j, :, rows] = dq_t[:, rows].T

        @pl.when(s == 0)
        def _():
            out_copy(dq, j, dq_send, dq_recv).start()

    for j in range(half):
        sibling_copy(j).wait_recv()
        back = grecv.at[:, j]
        pltpu.make_async_copy(back, back, gr_recv.at[j]).wait()
        for i, grad in enumerate((akg, avg)):
            mine = acc[j, i, block(2 + core)] + grecv[core, j, i].astype(jnp.float32)
            grad[:, cols(core * half + j, d)] = mine.astype(jnp.bfloat16)
            mine = srecv[j, i] + grecv[other, j, i].astype(jnp.float32)
            grad[:, cols(other * half + j, d)] = mine.astype(jnp.bfloat16)
    for j in range(half):
        terms = precv.at[:, j]
        pltpu.make_async_copy(terms, terms, pr_recv.at[j]).wait()
        for t in range(2):
            lanes = slice((t * half + j) * d, (t * half + j + 1) * d)
            for i, grad in enumerate((pkg, pvg)):
                grad[:, lanes] = jnp.sum(precv[t, j, :, i].astype(jnp.float32), axis=0)

    w_cross.wait_send()
    sent = pgath.at[:, pl.ds(0, n - 1)]
    pltpu.make_async_copy(sent, sent, pg_send).wait()
    for j in range(half):
        pltpu.make_async_copy(qog.at[1, j], qog.at[1, j], xq_send.at[j]).wait()
        mine = kall.at[j, :, block(2 + core)]
        pltpu.make_async_copy(mine, mine, xk_send.at[j]).wait()
        window = kall.at[j, :, pl.ds(prompt, 2 * height)]
        pltpu.make_async_copy(window, window, win_send.at[j]).wait()
        sent = psend.at[j, pl.ds(0, n - 1)]
        pltpu.make_async_copy(sent, sent, pr_send.at[j]).wait()
        pltpu.make_async_copy(gsend.at[j], gsend.at[j], gs_send.at[j]).wait()
        sibling_copy(j).wait_send()
        out_copy(attn, j, at_send, at_recv).wait()
        out_copy(dq, j, dq_send, dq_recv).wait()


def write_out(kv_heads, span, attn, dq, akg, avg, pkg, pvg, *refs):
    outs, (wide_sem, sem) = refs[:6], refs[6:]
    half = kv_heads // 2
    core = lax.rem(lax.axis_index("row"), 2)
    copies = [
        pltpu.make_async_copy(
            v.at[1 + t, j],
            out.at[:, pl.ds(pl.multiple_of((jnp.abs(core - t) * half + j) * span, span), span)],
            wide_sem.at[i, t, j],
        )
        for i, (v, out) in enumerate(((attn, outs[0]), (dq, outs[1])))
        for t in range(2)
        for j in range(half)
    ] + [
        pltpu.make_async_copy(v, out, sem.at[i])
        for i, (v, out) in enumerate(zip((akg, avg, pkg, pvg), outs[2:]))
    ]
    for copy in copies:
        copy.start()
    for copy in copies:
        copy.wait()


def per_device(n, queries, answer_keys, answer_values, prompt_keys, prompt_values, out_grad, weights, lengths):
    height = queries.shape[0]
    d = HEAD_DIM
    columns = answer_keys.shape[1]
    kv_heads = columns // d
    half = kv_heads // 2
    chips = n // 2
    group = queries.shape[1] // columns
    own_prompt = prompt_keys.shape[0]
    keys = own_prompt * n + 3 * height
    held = own_prompt * n + 4 * height
    span = group * d
    answers = lengths.shape[0]
    bf16, f32 = jnp.bfloat16, jnp.float32
    vmem = pl.BlockSpec(memory_space=pltpu.VMEM)
    hbm = pl.BlockSpec(memory_space=pltpu.HBM)
    dma = pltpu.SemaphoreType.DMA
    results = pl.pallas_call(
        functools.partial(kernel, n, kv_heads, group),
        out_shape=(
            pltpu.VMEM((3, half, height, span), bf16),
            pltpu.VMEM((3, half, height, span), bf16),
            pltpu.VMEM(answer_keys.shape, bf16),
            pltpu.VMEM(answer_keys.shape, bf16),
            pltpu.VMEM(prompt_keys.shape, f32),
            pltpu.VMEM(prompt_keys.shape, f32),
        ),
        in_specs=[hbm] * 8,
        out_specs=(vmem,) * 6,
        scratch_shapes=[
            pltpu.VMEM((2, half, 2, height, span), bf16),
            pltpu.VMEM((half, 2, held, d), bf16),
            pltpu.VMEM((d, keys), bf16),
            pltpu.VMEM((d, keys), bf16),
            pltpu.VMEM((2, n, own_prompt, half * d), bf16),
            pltpu.VMEM((2, 1, height), f32),
            pltpu.VMEM((1, answers), jnp.int32),
            pltpu.VMEM((2, half, d, group * height), bf16),
            pltpu.VMEM((group * height, d), bf16),
            pltpu.VMEM((2, half, d, group * height), bf16),
            pltpu.VMEM((2, half, keys, group * height), bf16),
            pltpu.VMEM((2, half, keys, group * height), bf16),
            pltpu.VMEM((half, 2, held, d), f32),
            pltpu.VMEM((half, n, 2, own_prompt, d), bf16),
            pltpu.VMEM((2, half, chips, 2, own_prompt, d), bf16),
            pltpu.VMEM((half, 2, 2, height, d), bf16),
            pltpu.VMEM((2, half, 2, height, d), bf16),
            pltpu.VMEM((half, 2, height, d), f32),
            pltpu.VMEM((2, 2, height, height), f32),
            pltpu.VMEM((height, height), bf16),
            dma((2,)),
            dma((half,)), dma((half,)), dma((half,)), dma((half,)), dma((half,)),
            dma,
            dma((half,)), dma((half,)), dma((half,)), dma((half,)), dma((half,)),
            dma,
            dma((half,)), dma((half,)), dma((half,)),
            dma,
            dma((half,)), dma((half,)), dma((half,)), dma((half,)), dma((half,)),
            dma, dma,
        ],
        compiler_params=pltpu.CompilerParams(
            collective_id=0, has_side_effects=True, vmem_limit_bytes=60 * 1024 * 1024
        ),
    )(
        queries, out_grad, answer_keys, answer_values, prompt_keys, prompt_values,
        weights.reshape(1, height), lengths.reshape(1, answers),
    )
    return pl.pallas_call(
        functools.partial(write_out, kv_heads, span),
        out_shape=(
            jax.ShapeDtypeStruct(queries.shape, bf16),
            jax.ShapeDtypeStruct(queries.shape, bf16),
            jax.ShapeDtypeStruct(answer_keys.shape, bf16),
            jax.ShapeDtypeStruct(answer_keys.shape, bf16),
            jax.ShapeDtypeStruct(prompt_keys.shape, f32),
            jax.ShapeDtypeStruct(prompt_keys.shape, f32),
        ),
        in_specs=[vmem] * 6,
        out_specs=(hbm,) * 6,
        scratch_shapes=[dma((2, 2, half)), dma((4,))],
        compiler_params=pltpu.CompilerParams(vmem_limit_bytes=8 * 1024 * 1024),
    )(*results)


def solution(mesh):
    both = ("grp", "row")
    wide = P(both, None)
    return jax.shard_map(
        functools.partial(per_device, mesh.shape["row"]),
        mesh=mesh,
        in_specs=(wide,) * 6 + (P(both), P("grp")),
        out_specs=(wide,) * 6,
        check_vma=False,
    )
```

```python
import functools
import math

import jax
import jax.numpy as jnp
from jax import lax
from jax.experimental import pallas as pl
from jax.experimental.pallas import tpu as pltpu
from jax.sharding import PartitionSpec as P

HEAD_DIM = 128
MASKED = -1e30
MESH = pl.DeviceIdType.MESH


def dot(a, b):
    return jnp.dot(a, b, preferred_element_type=jnp.float32)


def twice(x):
    return jnp.concatenate([x, x], axis=1)


def kernel(
    n, kv_heads, group,
    q_hbm, og_hbm, ak, av, pk, pv, w, lens,
    attn, dq, akg, avg, pkg, pvg,
    qog, kall, vt, kt, pgath, wst, lst, qs_t, cots, cots_t, p_all, ds_all, acc,
    psend, precv, gsend, grecv, srecv, bias, tri_b,
    small_sem, in_sem, kv_sem, xq_recv, xk_recv, win_recv, pg_recv, pr_recv, gr_recv, sr_recv, at_recv, dq_recv,
    xq_send, xk_send, win_send, pg_send, pr_send, gs_send, sr_send, at_send, dq_send, w_recv, w_send,
):
    me = lax.axis_index("row")
    height = ak.shape[0]
    d = HEAD_DIM
    span = group * d
    half = kv_heads // 2
    own_prompt = pk.shape[0]
    prompt = own_prompt * n
    factor = d ** (-0.5)
    log_factor = factor * math.log2(math.e)
    chips = n // 2
    core = lax.rem(me, 2)
    other = 1 - core
    chip = me // 2
    sibling = me + 1 - 2 * core
    after = lax.rem(chip + 1, chips)
    before = lax.rem(chip + chips - 1, chips)
    at1, at2, at3 = prompt, prompt + height, prompt + 2 * height

    def remote(src, dst, send, recv, target):
        return pltpu.make_async_remote_copy(
            src_ref=src, dst_ref=dst, send_sem=send, recv_sem=recv,
            device_id={"row": target}, device_id_type=MESH,
        )

    def cols(at, width):
        return pl.ds(pl.multiple_of(at * width, width), width)

    def block(b):
        return pl.ds(pl.multiple_of(prompt + b * height, height), height)

    def in_copies(j):
        head = core * half + j
        return (
            pltpu.make_async_copy(q_hbm.at[:, cols(head, span)], qog.at[1, j, 0], in_sem.at[j]),
            pltpu.make_async_copy(og_hbm.at[:, cols(head, span)], qog.at[1, j, 1], in_sem.at[j]),
        )

    def cross_copies(j):
        head = other * half + j
        return (
            remote(og_hbm.at[:, cols(head, span)], qog.at[0, j, 1], xq_send.at[j], xq_recv.at[j], sibling),
            remote(q_hbm.at[:, cols(head, span)], qog.at[0, j, 0], xq_send.at[j], xq_recv.at[j], sibling),
        )

    def kv_copies(j):
        head = core * half + j
        return [
            pltpu.make_async_copy(src.at[:, cols(head, d)], kall.at[j, i, block(2 + core)], kv_sem.at[j])
            for i, src in enumerate((ak, av))
        ]

    def kv_cross(j):
        head = other * half + j
        return [
            remote(src.at[:, cols(head, d)], kall.at[j, i, block(2 + core)], xk_send.at[j], xk_recv.at[j], sibling)
            for i, src in enumerate((ak, av))
        ]

    def win_copies(j):
        return [
            remote(
                src.at[:, pl.ds((t * half + j) * d, d)], kall.at[j, i, block(core)],
                win_send.at[j], win_recv.at[j], 2 * after + t,
            )
            for i, src in enumerate((ak, av)) for t in range(2)
        ]

    def prompt_copy(k, i):
        target = lax.rem(me + k, n)
        return remote(
            (pk, pv)[i].at[:, cols(lax.rem(target, 2), half * d)], pgath.at[i, me],
            pg_send, pg_recv, target,
        )

    def reduce_copy(j, k):
        target = lax.rem(me + k, n)
        return remote(psend.at[j, target], precv.at[core, j, chip], pr_send.at[j], pr_recv.at[j], target)

    def back_copy(j, t):
        return remote(gsend.at[j, t], grecv.at[core, j], gs_send.at[j], gr_recv.at[j], 2 * before + t)

    def sibling_copy(j):
        return remote(acc.at[j, :, block(2 + other)], srecv.at[j], sr_send.at[j], sr_recv.at[j], sibling)

    def out_copy(ref, j, send, recv):
        return remote(ref.at[0, j], ref.at[2, j], send.at[j], recv.at[j], sibling)

    barrier = pltpu.get_barrier_semaphore()

    @pl.loop(1, n)
    def _(k):
        pl.semaphore_signal(barrier, inc=1, device_id={"row": lax.rem(me + k, n)}, device_id_type=MESH)

    w_local = pltpu.make_async_copy(w, wst.at[1], small_sem.at[0])
    lens_local = pltpu.make_async_copy(lens, lst, small_sem.at[1])
    own_prompts = [
        pltpu.make_async_copy((pk, pv)[i].at[:, cols(core, half * d)], pgath.at[i, me], pg_recv) for i in range(2)
    ]
    w_local.start()
    lens_local.start()
    for j in range(half):
        for copy in in_copies(j):
            copy.start()
    for j in range(half):
        for copy in kv_copies(j):
            copy.start()
    for copy in own_prompts:
        copy.start()
    pl.semaphore_wait(barrier, n - 1)

    @pl.loop(1, n)
    def _(k):
        for i in range(2):
            prompt_copy(k, i).start()

    def send_window(j):
        @pl.when(chip < chips - 1)
        def _():
            for copy in win_copies(j):
                copy.start()

    w_cross = remote(w, wst.at[0], w_send, w_recv, sibling)
    w_cross.start()
    send_window(0)
    for j in range(half):
        for copy in cross_copies(j):
            copy.start()
        for copy in kv_cross(j):
            copy.start()

    acc[...] = jnp.zeros(acc.shape, jnp.float32)

    @pl.when(chip == 0)
    def _():
        kall[:, :, prompt : prompt + 2 * height] = jnp.zeros((half, 2, 2 * height, d), jnp.bfloat16)

    @pl.when(chip == chips - 1)
    def _():
        grecv[...] = jnp.zeros(grecv.shape, jnp.bfloat16)

    lens_local.wait()
    answers = lens.shape[1]
    row = lax.broadcasted_iota(jnp.int32, (answers, answers), 0)
    col = lax.broadcasted_iota(jnp.int32, (answers, answers), 1)
    starts = jnp.sum(
        jnp.where(col < row, jnp.broadcast_to(lst[...], (answers, answers)), 0),
        axis=1, keepdims=True,
    )
    key = lax.broadcasted_iota(jnp.int32, (height, height), 0)
    query = lax.broadcasted_iota(jnp.int32, (height, height), 1)
    tri = key <= query
    for b in range(2):
        base = (2 * chip + b) * height
        pos = base + lax.broadcasted_iota(jnp.int32, (1, height), 1)
        first = jnp.max(jnp.where(starts <= pos, starts, 0), axis=0, keepdims=True)
        bias[b, 0] = jnp.where(key + (base - height) >= first, 0.0, MASKED)
        both = jnp.where(tri, key + base, key + (base - 2 * height))
        bias[b, 1] = jnp.where(both >= first, 0.0, MASKED)
    tri_b[...] = tri.astype(jnp.float32).astype(jnp.bfloat16)

    def prepare(s, j):
        for h in range(group):
            rows = slice(h * height, (h + 1) * height)
            og_t = qog[s, j, 1, :, rows].T
            cots_t[s, j, :, rows] = (wst[s] * og_t.astype(jnp.float32)).astype(jnp.bfloat16)
            qs_t[s, j, :, rows] = qog[s, j, 0, :, rows].T

    w_local.wait()

    @pl.loop(0, half)
    def _(j):
        pltpu.make_async_copy(qog.at[1, j], qog.at[1, j], in_sem.at[j]).wait()
        prepare(1, j)

    w_cross.wait_recv()

    @pl.loop(0, half)
    def _(j):
        pltpu.make_async_copy(qog.at[0, j], qog.at[0, j], xq_recv.at[j]).wait()
        prepare(0, j)

    pltpu.make_async_copy(pgath, pgath, pg_recv).wait()
    for j in range(1, half):
        send_window(j)

    @pl.loop(0, 2 * half)
    def _(u):
        j = u // 2
        s = lax.rem(u, 2)
        b = s * core + (1 - s) * other

        @pl.when(s == 0)
        def _():
            mine = kall.at[j, :, block(2 + core)]
            pltpu.make_async_copy(mine, mine, kv_sem.at[j]).wait()
            theirs = kall.at[j, :, block(2 + other)]
            pltpu.make_async_copy(theirs, theirs, xk_recv.at[j]).wait()

            @pl.when(chip > 0)
            def _():
                window = kall.at[j, :, pl.ds(prompt, 2 * height)]
                pltpu.make_async_copy(window, window, win_recv.at[j]).wait()

            for i in range(2):
                gathered = pgath[i, :, :, cols(j, d)].astype(jnp.float32).reshape(prompt, d)
                kall[j, i, :prompt, :] = gathered.astype(jnp.bfloat16)

        near_far = pl.ds(pl.multiple_of(prompt + b * height, height), 3 * height)
        tri2 = twice(tri)
        keys = jnp.concatenate([kall[j, 0, :prompt], kall[j, 0, near_far]], axis=0)
        values = jnp.concatenate([kall[j, 1, :prompt], kall[j, 1, near_far]], axis=0)
        vt[...] = values.T
        for pair in range(group // 2):
            rows = slice(pair * 2 * height, (pair + 1) * 2 * height)
            scores = dot(keys, qs_t[s, j, :, rows])
            s_p = scores[:at1]
            s_n = scores[at2:at3] + twice(bias[b, 0])
            s_c = jnp.where(tri2, scores[at3:], scores[at1:at2]) + twice(bias[b, 1])
            top = jnp.maximum(
                jnp.maximum(jnp.max(s_p, axis=0, keepdims=True), jnp.max(s_n, axis=0, keepdims=True)),
                jnp.max(s_c, axis=0, keepdims=True),
            )
            e_p = jnp.exp2((s_p - top) * log_factor)
            e_n = jnp.exp2((s_n - top) * log_factor)
            e_c = jnp.exp2((s_c - top) * log_factor)
            total = (
                jnp.sum(e_p, axis=0, keepdims=True)
                + jnp.sum(e_n, axis=0, keepdims=True)
                + jnp.sum(e_c, axis=0, keepdims=True)
            )
            inv = 1.0 / total
            p_all[s, j, :at1, rows] = e_p.astype(jnp.bfloat16)
            p_all[s, j, at2:at3, rows] = e_n.astype(jnp.bfloat16)
            b_c = e_c.astype(jnp.bfloat16)
            b_d = b_c * twice(tri_b[...])
            p_all[s, j, at1:at2, rows] = b_c - b_d
            p_all[s, j, at3:, rows] = b_d
            out_t = (dot(vt[...], p_all[s, j, :, rows]) * inv).astype(jnp.bfloat16)
            cot_t = (cots_t[s, j, :, rows].astype(jnp.float32) * inv).astype(jnp.bfloat16)
            delta = jnp.sum(
                cot_t.astype(jnp.float32) * out_t.astype(jnp.float32), axis=0, keepdims=True
            )
            slopes = dot(values, cot_t)
            ds_all[s, j, :, rows] = (
                p_all[s, j, :, rows].astype(jnp.float32) * (slopes - delta)
            ).astype(jnp.bfloat16)
            cots[rows, :] = cot_t.T
            out = out_t.T
            for h in range(2):
                lanes = slice((2 * pair + h) * d, (2 * pair + h + 1) * d)
                attn[s, j, :, lanes] = out[h * height : (h + 1) * height]

        q_rows = jnp.concatenate([qog[s, j, 0, :, h * d : (h + 1) * d] for h in range(group)], axis=0)
        for i in range(2):
            part = dot(ds_all[s, j], q_rows) * factor if i == 0 else dot(p_all[s, j], cots[...])
            acc[j, i, :prompt] += part[:at1]
            acc[j, i, near_far] += part[at1:]

        @pl.when(s == 0)
        def _():
            out_copy(attn, j, at_send, at_recv).start()

        @pl.when(s == 1)
        def _():
            for i in range(2):
                psend[j, :, i] = acc[j, i, :prompt].reshape(n, own_prompt, d).astype(jnp.bfloat16)
                for t in range(2):
                    gsend[j, t, i] = acc[j, i, prompt + t * height : prompt + (t + 1) * height].astype(jnp.bfloat16)

            @pl.loop(1, n)
            def _(k):
                reduce_copy(j, k).start()

            pltpu.make_async_copy(psend.at[j, me], precv.at[core, j, chip], pr_recv.at[j]).start()

            @pl.when(chip > 0)
            def _():
                for t in range(2):
                    back_copy(j, t).start()

            sibling_copy(j).start()

    @pl.loop(0, 2 * half)
    def _(u):
        s = u // half
        j = lax.rem(u, half)
        b = s * core + (1 - s) * other
        near_far = pl.ds(pl.multiple_of(prompt + b * height, height), 3 * height)
        kt[:, :at1] = kall[j, 0, :prompt].T
        kt[:, at1:] = kall[j, 0, near_far].T
        dq_t = (dot(kt[...], ds_all[s, j]) * factor).astype(jnp.bfloat16)
        for h in range(group):
            rows = slice(h * height, (h + 1) * height)
            dq[s, j, :, rows] = dq_t[:, rows].T

        @pl.when(s == 0)
        def _():
            out_copy(dq, j, dq_send, dq_recv).start()

    for j in range(half):
        sibling_copy(j).wait_recv()

        @pl.when(chip < chips - 1)
        def _():
            back = grecv.at[:, j]
            pltpu.make_async_copy(back, back, gr_recv.at[j]).wait()

        for i, grad in enumerate((akg, avg)):
            mine = acc[j, i, block(2 + core)] + grecv[core, j, i].astype(jnp.float32)
            grad[:, cols(core * half + j, d)] = mine.astype(jnp.bfloat16)
            mine = srecv[j, i] + grecv[other, j, i].astype(jnp.float32)
            grad[:, cols(other * half + j, d)] = mine.astype(jnp.bfloat16)
    for j in range(half):
        terms = precv.at[:, j]
        pltpu.make_async_copy(terms, terms, pr_recv.at[j]).wait()
        for t in range(2):
            lanes = slice((t * half + j) * d, (t * half + j + 1) * d)
            for i, grad in enumerate((pkg, pvg)):
                grad[:, lanes] = jnp.sum(precv[t, j, :, i].astype(jnp.float32), axis=0)

    w_cross.wait_send()
    sent = pgath.at[:, pl.ds(0, n - 1)]
    pltpu.make_async_copy(sent, sent, pg_send).wait()
    for j in range(half):
        pltpu.make_async_copy(qog.at[1, j], qog.at[1, j], xq_send.at[j]).wait()
        mine = kall.at[j, :, block(2 + core)]
        pltpu.make_async_copy(mine, mine, xk_send.at[j]).wait()

        @pl.when(chip < chips - 1)
        def _():
            window = kall.at[j, :, pl.ds(prompt, 2 * height)]
            pltpu.make_async_copy(window, window, win_send.at[j]).wait()

        @pl.when(chip > 0)
        def _():
            pltpu.make_async_copy(gsend.at[j], gsend.at[j], gs_send.at[j]).wait()

        sent = psend.at[j, pl.ds(0, n - 1)]
        pltpu.make_async_copy(sent, sent, pr_send.at[j]).wait()
        sibling_copy(j).wait_send()
        out_copy(attn, j, at_send, at_recv).wait()
        out_copy(dq, j, dq_send, dq_recv).wait()


def write_out(kv_heads, span, attn, dq, akg, avg, pkg, pvg, *refs):
    outs, (wide_sem, sem) = refs[:6], refs[6:]
    half = kv_heads // 2
    core = lax.rem(lax.axis_index("row"), 2)
    copies = [
        pltpu.make_async_copy(
            v.at[1 + t, j],
            out.at[:, pl.ds(pl.multiple_of((jnp.abs(core - t) * half + j) * span, span), span)],
            wide_sem.at[i, t, j],
        )
        for i, (v, out) in enumerate(((attn, outs[0]), (dq, outs[1])))
        for t in range(2)
        for j in range(half)
    ] + [
        pltpu.make_async_copy(v, out, sem.at[i])
        for i, (v, out) in enumerate(zip((akg, avg, pkg, pvg), outs[2:]))
    ]
    for copy in copies:
        copy.start()
    for copy in copies:
        copy.wait()


def per_device(n, queries, answer_keys, answer_values, prompt_keys, prompt_values, out_grad, weights, lengths):
    height = queries.shape[0]
    d = HEAD_DIM
    columns = answer_keys.shape[1]
    kv_heads = columns // d
    half = kv_heads // 2
    chips = n // 2
    group = queries.shape[1] // columns
    own_prompt = prompt_keys.shape[0]
    keys = own_prompt * n + 3 * height
    held = own_prompt * n + 4 * height
    span = group * d
    answers = lengths.shape[0]
    bf16, f32 = jnp.bfloat16, jnp.float32
    vmem = pl.BlockSpec(memory_space=pltpu.VMEM)
    hbm = pl.BlockSpec(memory_space=pltpu.HBM)
    dma = pltpu.SemaphoreType.DMA
    results = pl.pallas_call(
        functools.partial(kernel, n, kv_heads, group),
        out_shape=(
            pltpu.VMEM((3, half, height, span), bf16),
            pltpu.VMEM((3, half, height, span), bf16),
            pltpu.VMEM(answer_keys.shape, bf16),
            pltpu.VMEM(answer_keys.shape, bf16),
            pltpu.VMEM(prompt_keys.shape, f32),
            pltpu.VMEM(prompt_keys.shape, f32),
        ),
        in_specs=[hbm] * 8,
        out_specs=(vmem,) * 6,
        scratch_shapes=[
            pltpu.VMEM((2, half, 2, height, span), bf16),
            pltpu.VMEM((half, 2, held, d), bf16),
            pltpu.VMEM((d, keys), bf16),
            pltpu.VMEM((d, keys), bf16),
            pltpu.VMEM((2, n, own_prompt, half * d), bf16),
            pltpu.VMEM((2, 1, height), f32),
            pltpu.VMEM((1, answers), jnp.int32),
            pltpu.VMEM((2, half, d, group * height), bf16),
            pltpu.VMEM((group * height, d), bf16),
            pltpu.VMEM((2, half, d, group * height), bf16),
            pltpu.VMEM((2, half, keys, group * height), bf16),
            pltpu.VMEM((2, half, keys, group * height), bf16),
            pltpu.VMEM((half, 2, held, d), f32),
            pltpu.VMEM((half, n, 2, own_prompt, d), bf16),
            pltpu.VMEM((2, half, chips, 2, own_prompt, d), bf16),
            pltpu.VMEM((half, 2, 2, height, d), bf16),
            pltpu.VMEM((2, half, 2, height, d), bf16),
            pltpu.VMEM((half, 2, height, d), f32),
            pltpu.VMEM((2, 2, height, height), f32),
            pltpu.VMEM((height, height), bf16),
            dma((2,)),
            dma((half,)), dma((half,)), dma((half,)), dma((half,)), dma((half,)),
            dma,
            dma((half,)), dma((half,)), dma((half,)), dma((half,)), dma((half,)),
            dma((half,)), dma((half,)), dma((half,)),
            dma,
            dma((half,)), dma((half,)), dma((half,)), dma((half,)), dma((half,)),
            dma, dma,
        ],
        compiler_params=pltpu.CompilerParams(
            collective_id=0, has_side_effects=True, vmem_limit_bytes=60 * 1024 * 1024
        ),
    )(
        queries, out_grad, answer_keys, answer_values, prompt_keys, prompt_values,
        weights.reshape(1, height), lengths.reshape(1, answers),
    )
    return pl.pallas_call(
        functools.partial(write_out, kv_heads, span),
        out_shape=(
            jax.ShapeDtypeStruct(queries.shape, bf16),
            jax.ShapeDtypeStruct(queries.shape, bf16),
            jax.ShapeDtypeStruct(answer_keys.shape, bf16),
            jax.ShapeDtypeStruct(answer_keys.shape, bf16),
            jax.ShapeDtypeStruct(prompt_keys.shape, f32),
            jax.ShapeDtypeStruct(prompt_keys.shape, f32),
        ),
        in_specs=[vmem] * 6,
        out_specs=(hbm,) * 6,
        scratch_shapes=[dma((2, 2, half)), dma((4,))],
        compiler_params=pltpu.CompilerParams(vmem_limit_bytes=8 * 1024 * 1024),
    )(*results)


def solution(mesh):
    both = ("grp", "row")
    wide = P(both, None)
    return jax.shard_map(
        functools.partial(per_device, mesh.shape["row"]),
        mesh=mesh,
        in_specs=(wide,) * 6 + (P(both), P("grp")),
        out_specs=(wide,) * 6,
        check_vma=False,
    )
```

```python
import functools
import math

import jax
import jax.numpy as jnp
from jax import lax
from jax.experimental import pallas as pl
from jax.experimental.pallas import tpu as pltpu
from jax.sharding import PartitionSpec as P

HEAD_DIM = 128
MASKED = -1e30
MESH = pl.DeviceIdType.MESH


def dot(a, b):
    return jnp.dot(a, b, preferred_element_type=jnp.float32)


def twice(x):
    return jnp.concatenate([x, x], axis=1)


def kernel(
    n, kv_heads, group,
    q_hbm, og_hbm, ak, av, pk, pv, w, lens,
    attn, dq, akg, avg, pkg, pvg,
    qog, kall, vt, kt, pgath, wst, lst, qs_t, cots, cots_t, p_all, ds_all, acc,
    psend, precv, gsend, grecv, srecv, bias, tri_b,
    small_sem, in_sem, kv_sem, xq_recv, xk_recv, win_recv, pg_recv, pr_recv, gr_recv, sr_recv, at_recv, dq_recv,
    xq_send, xk_send, win_send, pg_send, pr_send, gs_send, sr_send, at_send, dq_send, w_recv, w_send,
):
    me = lax.axis_index("row")
    height = ak.shape[0]
    d = HEAD_DIM
    span = group * d
    half = kv_heads // 2
    own_prompt = pk.shape[0]
    prompt = own_prompt * n
    factor = d ** (-0.5)
    log_factor = factor * math.log2(math.e)
    chips = n // 2
    core = lax.rem(me, 2)
    other = 1 - core
    chip = me // 2
    sibling = me + 1 - 2 * core
    after = lax.rem(chip + 1, chips)
    before = lax.rem(chip + chips - 1, chips)
    at1, at2, at3 = prompt, prompt + height, prompt + 2 * height

    def remote(src, dst, send, recv, target):
        return pltpu.make_async_remote_copy(
            src_ref=src, dst_ref=dst, send_sem=send, recv_sem=recv,
            device_id={"row": target}, device_id_type=MESH,
        )

    def cols(at, width):
        return pl.ds(pl.multiple_of(at * width, width), width)

    def block(b):
        return pl.ds(pl.multiple_of(prompt + b * height, height), height)

    def in_copies(j):
        head = core * half + j
        return (
            pltpu.make_async_copy(q_hbm.at[:, cols(head, span)], qog.at[1, j, 0], in_sem.at[j]),
            pltpu.make_async_copy(og_hbm.at[:, cols(head, span)], qog.at[1, j, 1], in_sem.at[j]),
        )

    def cross_copies(j):
        head = other * half + j
        return (
            remote(og_hbm.at[:, cols(head, span)], qog.at[0, j, 1], xq_send.at[j], xq_recv.at[j], sibling),
            remote(q_hbm.at[:, cols(head, span)], qog.at[0, j, 0], xq_send.at[j], xq_recv.at[j], sibling),
        )

    def kv_copies(j):
        head = core * half + j
        return [
            pltpu.make_async_copy(src.at[:, cols(head, d)], kall.at[j, i, block(2 + core)], kv_sem.at[j])
            for i, src in enumerate((ak, av))
        ]

    def kv_cross(j):
        head = other * half + j
        return [
            remote(src.at[:, cols(head, d)], kall.at[j, i, block(2 + core)], xk_send.at[j], xk_recv.at[j], sibling)
            for i, src in enumerate((ak, av))
        ]

    def win_copies(j):
        return [
            remote(
                src.at[:, pl.ds((t * half + j) * d, d)], kall.at[j, i, block(core)],
                win_send.at[j], win_recv.at[j, core], 2 * after + t,
            )
            for i, src in enumerate((ak, av)) for t in range(2)
        ]

    def prompt_copy(j, k, i):
        target = lax.rem(me + k, n)
        return remote(
            (pk, pv)[i].at[:, cols(lax.rem(target, 2) * half + j, d)], pgath.at[j, i, me],
            pg_send.at[j], pg_recv.at[j], target,
        )

    def reduce_copy(j, k):
        target = lax.rem(me + k, n)
        return remote(psend.at[j, target], precv.at[core, j, chip], pr_send.at[j], pr_recv.at[j], target)

    def back_copy(j, t):
        return remote(gsend.at[j, t], grecv.at[core, j], gs_send.at[j], gr_recv.at[j], 2 * before + t)

    def sibling_copy(j):
        return remote(acc.at[j, :, block(2 + other)], srecv.at[j], sr_send.at[j], sr_recv.at[j], sibling)

    def out_copy(ref, j, send, recv):
        return remote(ref.at[0, j], ref.at[2, j], send.at[j], recv.at[j], sibling)

    barrier = pltpu.get_barrier_semaphore()

    @pl.loop(1, n)
    def _(k):
        pl.semaphore_signal(barrier, inc=1, device_id={"row": lax.rem(me + k, n)}, device_id_type=MESH)

    w_local = pltpu.make_async_copy(w, wst.at[1], small_sem.at[0])
    lens_local = pltpu.make_async_copy(lens, lst, small_sem.at[1])
    own_prompts = [
        pltpu.make_async_copy((pk, pv)[i].at[:, cols(core * half + j, d)], pgath.at[j, i, me], pg_recv.at[j])
        for j in range(half)
        for i in range(2)
    ]
    w_local.start()
    lens_local.start()
    for j in range(half):
        for copy in in_copies(j):
            copy.start()
    for j in range(half):
        for copy in kv_copies(j):
            copy.start()
    for copy in own_prompts:
        copy.start()
    pl.semaphore_wait(barrier, n - 1)

    def send_prompts(j):
        @pl.loop(1, n)
        def _(k):
            for i in range(2):
                prompt_copy(j, k, i).start()

    def send_window(j, condition):
        @pl.when(jnp.logical_and(chip < chips - 1, condition))
        def _():
            for copy in win_copies(j):
                copy.start()

    w_cross = remote(w, wst.at[0], w_send, w_recv, sibling)
    w_cross.start()
    for j in range(half):
        send_prompts(j)
        if j == 0:
            send_window(0, core == 1)
        for copy in cross_copies(j):
            copy.start()
        for copy in kv_cross(j):
            copy.start()

    acc[...] = jnp.zeros(acc.shape, jnp.float32)

    @pl.when(chip == 0)
    def _():
        kall[:, :, prompt : prompt + 2 * height] = jnp.zeros((half, 2, 2 * height, d), jnp.bfloat16)

    @pl.when(chip == chips - 1)
    def _():
        grecv[...] = jnp.zeros(grecv.shape, jnp.bfloat16)

    lens_local.wait()
    answers = lens.shape[1]
    row = lax.broadcasted_iota(jnp.int32, (answers, answers), 0)
    col = lax.broadcasted_iota(jnp.int32, (answers, answers), 1)
    starts = jnp.sum(
        jnp.where(col < row, jnp.broadcast_to(lst[...], (answers, answers)), 0),
        axis=1, keepdims=True,
    )
    key = lax.broadcasted_iota(jnp.int32, (height, height), 0)
    query = lax.broadcasted_iota(jnp.int32, (height, height), 1)
    tri = key <= query
    for b in range(2):
        base = (2 * chip + b) * height
        pos = base + lax.broadcasted_iota(jnp.int32, (1, height), 1)
        first = jnp.max(jnp.where(starts <= pos, starts, 0), axis=0, keepdims=True)
        bias[b, 0] = jnp.where(key + (base - height) >= first, 0.0, MASKED)
        both = jnp.where(tri, key + base, key + (base - 2 * height))
        bias[b, 1] = jnp.where(both >= first, 0.0, MASKED)
    tri_b[...] = tri.astype(jnp.float32).astype(jnp.bfloat16)

    def prepare(s, j):
        for h in range(group):
            rows = slice(h * height, (h + 1) * height)
            og_t = qog[s, j, 1, :, rows].T
            cots_t[s, j, :, rows] = (wst[s] * og_t.astype(jnp.float32)).astype(jnp.bfloat16)
            qs_t[s, j, :, rows] = qog[s, j, 0, :, rows].T

    w_local.wait()

    @pl.loop(0, half)
    def _(j):
        pltpu.make_async_copy(qog.at[1, j], qog.at[1, j], in_sem.at[j]).wait()
        prepare(1, j)

    send_window(0, core == 0)
    w_cross.wait_recv()

    @pl.loop(0, half)
    def _(j):
        pltpu.make_async_copy(qog.at[0, j], qog.at[0, j], xq_recv.at[j]).wait()
        prepare(0, j)

    pltpu.make_async_copy(pgath.at[0], pgath.at[0], pg_recv.at[0]).wait()
    for j in range(1, half):
        send_window(j, True)

    @pl.loop(0, 2 * half)
    def _(u):
        j = u // 2
        b = 1 - lax.rem(u, 2)
        s = b * core + (1 - b) * other

        @pl.when(b == 1)
        def _():
            mine = kall.at[j, :, block(2 + core)]
            pltpu.make_async_copy(mine, mine, kv_sem.at[j]).wait()
            theirs = kall.at[j, :, block(2 + other)]
            pltpu.make_async_copy(theirs, theirs, xk_recv.at[j]).wait()

            @pl.when(j > 0)
            def _():
                pltpu.make_async_copy(pgath.at[j], pgath.at[j], pg_recv.at[j]).wait()

            for i in range(2):
                gathered = pgath[j, i].astype(jnp.float32).reshape(prompt, d)
                kall[j, i, :prompt, :] = gathered.astype(jnp.bfloat16)

        @pl.when(chip > 0)
        def _():
            window = kall.at[j, :, block(b)]
            pltpu.make_async_copy(window, window, win_recv.at[j, b]).wait()

        near_far = pl.ds(pl.multiple_of(prompt + b * height, height), 3 * height)
        tri2 = twice(tri)
        keys = jnp.concatenate([kall[j, 0, :prompt], kall[j, 0, near_far]], axis=0)
        values = jnp.concatenate([kall[j, 1, :prompt], kall[j, 1, near_far]], axis=0)
        vt[...] = values.T
        held = {}

        def rows_of(pair):
            return slice(pair * 2 * height, (pair + 1) * 2 * height)

        def score(pair):
            scores = dot(keys, qs_t[s, j, :, rows_of(pair)])
            s_p = scores[:at1]
            s_n = scores[at2:at3] + twice(bias[b, 0])
            s_c = jnp.where(tri2, scores[at3:], scores[at1:at2]) + twice(bias[b, 1])
            top = jnp.maximum(
                jnp.maximum(jnp.max(s_p, axis=0, keepdims=True), jnp.max(s_n, axis=0, keepdims=True)),
                jnp.max(s_c, axis=0, keepdims=True),
            )
            held[pair] = s_p, s_n, s_c, top

        def soften(pair):
            rows = rows_of(pair)
            s_p, s_n, s_c, top = held[pair]
            e_p = jnp.exp2((s_p - top) * log_factor)
            e_n = jnp.exp2((s_n - top) * log_factor)
            e_c = jnp.exp2((s_c - top) * log_factor)
            total = (
                jnp.sum(e_p, axis=0, keepdims=True)
                + jnp.sum(e_n, axis=0, keepdims=True)
                + jnp.sum(e_c, axis=0, keepdims=True)
            )
            p_all[s, j, :at1, rows] = e_p.astype(jnp.bfloat16)
            p_all[s, j, at2:at3, rows] = e_n.astype(jnp.bfloat16)
            b_c = e_c.astype(jnp.bfloat16)
            b_d = b_c * twice(tri_b[...])
            p_all[s, j, at1:at2, rows] = b_c - b_d
            p_all[s, j, at3:, rows] = b_d
            held[pair] = 1.0 / total

        def attend(pair):
            rows = rows_of(pair)
            inv = held[pair]
            out_t = (dot(vt[...], p_all[s, j, :, rows]) * inv).astype(jnp.bfloat16)
            cot_t = (cots_t[s, j, :, rows].astype(jnp.float32) * inv).astype(jnp.bfloat16)
            delta = jnp.sum(
                cot_t.astype(jnp.float32) * out_t.astype(jnp.float32), axis=0, keepdims=True
            )
            cots[rows, :] = cot_t.T
            out = out_t.T
            for h in range(2):
                lanes = slice((2 * pair + h) * d, (2 * pair + h + 1) * d)
                attn[s, j, :, lanes] = out[h * height : (h + 1) * height]
            held[pair] = cot_t, delta

        def slope(pair):
            rows = rows_of(pair)
            cot_t, delta = held[pair]
            slopes = dot(values, cot_t)
            ds_all[s, j, :, rows] = p_all[s, j, :, rows] * (slopes - delta).astype(jnp.bfloat16)

        pairs = group // 2
        for step in range(-2, pairs + 2):
            if 0 <= step < pairs:
                soften(step)
            if 0 <= step + 2 < pairs:
                score(step + 2)
            if 0 <= step - 1 < pairs:
                attend(step - 1)
            if 0 <= step - 2 < pairs:
                slope(step - 2)

        q_rows = jnp.concatenate([qog[s, j, 0, :, h * d : (h + 1) * d] for h in range(group)], axis=0)
        for i in range(2):
            part = dot(ds_all[s, j], q_rows) * factor if i == 0 else dot(p_all[s, j], cots[...])
            acc[j, i, :prompt] += part[:at1]
            acc[j, i, near_far] += part[at1:]

        @pl.when(s == 0)
        def _():
            out_copy(attn, j, at_send, at_recv).start()

        @pl.when(b == 0)
        def _():
            for i in range(2):
                psend[j, :, i] = acc[j, i, :prompt].reshape(n, own_prompt, d).astype(jnp.bfloat16)
                for t in range(2):
                    gsend[j, t, i] = acc[j, i, prompt + t * height : prompt + (t + 1) * height].astype(jnp.bfloat16)

            @pl.loop(1, n)
            def _(k):
                reduce_copy(j, k).start()

            pltpu.make_async_copy(psend.at[j, me], precv.at[core, j, chip], pr_recv.at[j]).start()

            @pl.when(chip > 0)
            def _():
                for t in range(2):
                    back_copy(j, t).start()

            sibling_copy(j).start()

    @pl.loop(0, 2 * half)
    def _(u):
        s = u // half
        j = lax.rem(u, half)
        b = s * core + (1 - s) * other
        near_far = pl.ds(pl.multiple_of(prompt + b * height, height), 3 * height)
        kt[:, :at1] = kall[j, 0, :prompt].T
        kt[:, at1:] = kall[j, 0, near_far].T
        dq_t = (dot(kt[...], ds_all[s, j]) * factor).astype(jnp.bfloat16)
        for h in range(group):
            rows = slice(h * height, (h + 1) * height)
            dq[s, j, :, rows] = dq_t[:, rows].T

        @pl.when(s == 0)
        def _():
            out_copy(dq, j, dq_send, dq_recv).start()

    for j in range(half):
        sibling_copy(j).wait_recv()

        @pl.when(chip < chips - 1)
        def _():
            back = grecv.at[:, j]
            pltpu.make_async_copy(back, back, gr_recv.at[j]).wait()

        for i, grad in enumerate((akg, avg)):
            mine = acc[j, i, block(2 + core)] + grecv[core, j, i].astype(jnp.float32)
            grad[:, cols(core * half + j, d)] = mine.astype(jnp.bfloat16)
            mine = srecv[j, i] + grecv[other, j, i].astype(jnp.float32)
            grad[:, cols(other * half + j, d)] = mine.astype(jnp.bfloat16)
    for j in range(half):
        terms = precv.at[:, j]
        pltpu.make_async_copy(terms, terms, pr_recv.at[j]).wait()
        for t in range(2):
            lanes = slice((t * half + j) * d, (t * half + j + 1) * d)
            for i, grad in enumerate((pkg, pvg)):
                grad[:, lanes] = jnp.sum(precv[t, j, :, i].astype(jnp.float32), axis=0)

    w_cross.wait_send()
    for j in range(half):
        sent = pgath.at[j, :, pl.ds(0, n - 1)]
        pltpu.make_async_copy(sent, sent, pg_send.at[j]).wait()
        pltpu.make_async_copy(qog.at[1, j], qog.at[1, j], xq_send.at[j]).wait()
        mine = kall.at[j, :, block(2 + core)]
        pltpu.make_async_copy(mine, mine, xk_send.at[j]).wait()

        @pl.when(chip < chips - 1)
        def _():
            window = kall.at[j, :, pl.ds(prompt, 2 * height)]
            pltpu.make_async_copy(window, window, win_send.at[j]).wait()

        @pl.when(chip > 0)
        def _():
            pltpu.make_async_copy(gsend.at[j], gsend.at[j], gs_send.at[j]).wait()

        sent = psend.at[j, pl.ds(0, n - 1)]
        pltpu.make_async_copy(sent, sent, pr_send.at[j]).wait()
        sibling_copy(j).wait_send()
        out_copy(attn, j, at_send, at_recv).wait()
        out_copy(dq, j, dq_send, dq_recv).wait()


def write_out(kv_heads, span, attn, dq, akg, avg, pkg, pvg, *refs):
    outs, (wide_sem, sem) = refs[:6], refs[6:]
    half = kv_heads // 2
    core = lax.rem(lax.axis_index("row"), 2)
    copies = [
        pltpu.make_async_copy(
            v.at[1 + t, j],
            out.at[:, pl.ds(pl.multiple_of((jnp.abs(core - t) * half + j) * span, span), span)],
            wide_sem.at[i, t, j],
        )
        for i, (v, out) in enumerate(((attn, outs[0]), (dq, outs[1])))
        for t in range(2)
        for j in range(half)
    ] + [
        pltpu.make_async_copy(v, out, sem.at[i])
        for i, (v, out) in enumerate(zip((akg, avg, pkg, pvg), outs[2:]))
    ]
    for copy in copies:
        copy.start()
    for copy in copies:
        copy.wait()


def per_device(n, queries, answer_keys, answer_values, prompt_keys, prompt_values, out_grad, weights, lengths):
    height = queries.shape[0]
    d = HEAD_DIM
    columns = answer_keys.shape[1]
    kv_heads = columns // d
    half = kv_heads // 2
    chips = n // 2
    group = queries.shape[1] // columns
    own_prompt = prompt_keys.shape[0]
    keys = own_prompt * n + 3 * height
    held = own_prompt * n + 4 * height
    span = group * d
    answers = lengths.shape[0]
    bf16, f32 = jnp.bfloat16, jnp.float32
    vmem = pl.BlockSpec(memory_space=pltpu.VMEM)
    hbm = pl.BlockSpec(memory_space=pltpu.HBM)
    dma = pltpu.SemaphoreType.DMA
    results = pl.pallas_call(
        functools.partial(kernel, n, kv_heads, group),
        out_shape=(
            pltpu.VMEM((3, half, height, span), bf16),
            pltpu.VMEM((3, half, height, span), bf16),
            pltpu.VMEM(answer_keys.shape, bf16),
            pltpu.VMEM(answer_keys.shape, bf16),
            pltpu.VMEM(prompt_keys.shape, f32),
            pltpu.VMEM(prompt_keys.shape, f32),
        ),
        in_specs=[hbm] * 8,
        out_specs=(vmem,) * 6,
        scratch_shapes=[
            pltpu.VMEM((2, half, 2, height, span), bf16),
            pltpu.VMEM((half, 2, held, d), bf16),
            pltpu.VMEM((d, keys), bf16),
            pltpu.VMEM((d, keys), bf16),
            pltpu.VMEM((half, 2, n, own_prompt, d), bf16),
            pltpu.VMEM((2, 1, height), f32),
            pltpu.VMEM((1, answers), jnp.int32),
            pltpu.VMEM((2, half, d, group * height), bf16),
            pltpu.VMEM((group * height, d), bf16),
            pltpu.VMEM((2, half, d, group * height), bf16),
            pltpu.VMEM((2, half, keys, group * height), bf16),
            pltpu.VMEM((2, half, keys, group * height), bf16),
            pltpu.VMEM((half, 2, held, d), f32),
            pltpu.VMEM((half, n, 2, own_prompt, d), bf16),
            pltpu.VMEM((2, half, chips, 2, own_prompt, d), bf16),
            pltpu.VMEM((half, 2, 2, height, d), bf16),
            pltpu.VMEM((2, half, 2, height, d), bf16),
            pltpu.VMEM((half, 2, height, d), f32),
            pltpu.VMEM((2, 2, height, height), f32),
            pltpu.VMEM((height, height), bf16),
            dma((2,)),
            dma((half,)), dma((half,)), dma((half,)), dma((half,)),
            dma((half, 2)),
            *[dma((half,))] * 15,
            dma, dma,
        ],
        compiler_params=pltpu.CompilerParams(
            collective_id=0, has_side_effects=True, vmem_limit_bytes=60 * 1024 * 1024
        ),
    )(
        queries, out_grad, answer_keys, answer_values, prompt_keys, prompt_values,
        weights.reshape(1, height), lengths.reshape(1, answers),
    )
    return pl.pallas_call(
        functools.partial(write_out, kv_heads, span),
        out_shape=(
            jax.ShapeDtypeStruct(queries.shape, bf16),
            jax.ShapeDtypeStruct(queries.shape, bf16),
            jax.ShapeDtypeStruct(answer_keys.shape, bf16),
            jax.ShapeDtypeStruct(answer_keys.shape, bf16),
            jax.ShapeDtypeStruct(prompt_keys.shape, f32),
            jax.ShapeDtypeStruct(prompt_keys.shape, f32),
        ),
        in_specs=[vmem] * 6,
        out_specs=(hbm,) * 6,
        scratch_shapes=[dma((2, 2, half)), dma((4,))],
        compiler_params=pltpu.CompilerParams(vmem_limit_bytes=8 * 1024 * 1024),
    )(*results)


def solution(mesh):
    both = ("grp", "row")
    wide = P(both, None)
    return jax.shard_map(
        functools.partial(per_device, mesh.shape["row"]),
        mesh=mesh,
        in_specs=(wide,) * 6 + (P(both), P("grp")),
        out_specs=(wide,) * 6,
        check_vma=False,
    )
```

```python
import functools
import math

import jax
import jax.numpy as jnp
from jax import lax
from jax.experimental import pallas as pl
from jax.experimental.pallas import tpu as pltpu
from jax.sharding import PartitionSpec as P

HEAD_DIM = 128
MASKED = -1e30
MESH = pl.DeviceIdType.MESH


def dot(a, b):
    return jnp.dot(a, b, preferred_element_type=jnp.float32)


def twice(x):
    return jnp.concatenate([x, x], axis=1)


def kernel(
    n, kv_heads, group,
    q_hbm, og_hbm, ak, av, pk, pv, w, lens,
    attn, dq, akg, avg, pkg, pvg,
    qog, kall, vt, kt, pgath, wst, lst, qs_t, cots, cots_t, p_all, ds_all, acc,
    psend, precv, gsend, grecv, srecv, bias, tri_b,
    small_sem, in_sem, kv_sem, xq_recv, xk_recv, win_recv, pg_recv, pr_recv, gr_recv, sr_recv, at_recv, dq_recv,
    xq_send, xk_send, win_send, pg_send, pr_send, gs_send, sr_send, at_send, dq_send, w_recv, w_send,
):
    me = lax.axis_index("row")
    height = ak.shape[0]
    d = HEAD_DIM
    span = group * d
    half = kv_heads // 2
    own_prompt = pk.shape[0]
    prompt = own_prompt * n
    factor = d ** (-0.5)
    log_factor = factor * math.log2(math.e)
    chips = n // 2
    core = lax.rem(me, 2)
    other = 1 - core
    chip = me // 2
    sibling = me + 1 - 2 * core
    after = lax.rem(chip + 1, chips)
    before = lax.rem(chip + chips - 1, chips)
    at1, at2, at3 = prompt, prompt + height, prompt + 2 * height

    def remote(src, dst, send, recv, target):
        return pltpu.make_async_remote_copy(
            src_ref=src, dst_ref=dst, send_sem=send, recv_sem=recv,
            device_id={"row": target}, device_id_type=MESH,
        )

    def cols(at, width):
        return pl.ds(pl.multiple_of(at * width, width), width)

    def block(b):
        return pl.ds(pl.multiple_of(prompt + b * height, height), height)

    def in_copies(j):
        head = core * half + j
        return (
            pltpu.make_async_copy(q_hbm.at[:, cols(head, span)], qog.at[1, j, 0], in_sem.at[j]),
            pltpu.make_async_copy(og_hbm.at[:, cols(head, span)], qog.at[1, j, 1], in_sem.at[j]),
        )

    def cross_copies(j):
        head = other * half + j
        return (
            remote(og_hbm.at[:, cols(head, span)], qog.at[0, j, 1], xq_send.at[j], xq_recv.at[j], sibling),
            remote(q_hbm.at[:, cols(head, span)], qog.at[0, j, 0], xq_send.at[j], xq_recv.at[j], sibling),
        )

    def kv_copies(j):
        head = core * half + j
        return [
            pltpu.make_async_copy(src.at[:, cols(head, d)], kall.at[j, i, block(2 + core)], kv_sem.at[j])
            for i, src in enumerate((ak, av))
        ]

    def kv_cross(j):
        head = other * half + j
        return [
            remote(src.at[:, cols(head, d)], kall.at[j, i, block(2 + core)], xk_send.at[j], xk_recv.at[j], sibling)
            for i, src in enumerate((ak, av))
        ]

    def win_copies(j):
        return [
            remote(
                src.at[:, pl.ds((t * half + j) * d, d)], kall.at[j, i, block(core)],
                win_send.at[j], win_recv.at[j, core], 2 * after + t,
            )
            for i, src in enumerate((ak, av)) for t in range(2)
        ]

    def prompt_copy(j, k, i):
        target = lax.rem(me + k, n)
        return remote(
            (pk, pv)[i].at[:, cols(lax.rem(target, 2) * half + j, d)], pgath.at[j, i, me],
            pg_send.at[j], pg_recv.at[j], target,
        )

    def reduce_copy(j, k):
        target = lax.rem(me + k, n)
        return remote(psend.at[j, target], precv.at[core, j, chip], pr_send.at[j], pr_recv.at[j], target)

    def back_copy(j, t):
        return remote(gsend.at[j, t], grecv.at[core, j], gs_send.at[j, t], gr_recv.at[j], 2 * before + t)

    def send_back(j, t):
        for i in range(2):
            gsend[j, t, i] = acc[j, i, prompt + t * height : prompt + (t + 1) * height].astype(jnp.bfloat16)

        @pl.when(chip > 0)
        def _():
            back_copy(j, t).start()

    def sibling_copy(j):
        return remote(acc.at[j, :, block(2 + other)], srecv.at[j], sr_send.at[j], sr_recv.at[j], sibling)

    def out_copy(ref, j, send, recv):
        return remote(ref.at[0, j], ref.at[2, j], send.at[j], recv.at[j], sibling)

    barrier = pltpu.get_barrier_semaphore()

    @pl.loop(1, n)
    def _(k):
        pl.semaphore_signal(barrier, inc=1, device_id={"row": lax.rem(me + k, n)}, device_id_type=MESH)

    w_local = pltpu.make_async_copy(w, wst.at[1], small_sem.at[0])
    lens_local = pltpu.make_async_copy(lens, lst, small_sem.at[1])
    own_prompts = [
        pltpu.make_async_copy((pk, pv)[i].at[:, cols(core * half + j, d)], pgath.at[j, i, me], pg_recv.at[j])
        for j in range(half)
        for i in range(2)
    ]
    w_local.start()
    lens_local.start()
    for j in range(half):
        for copy in in_copies(j):
            copy.start()
    for j in range(half):
        for copy in kv_copies(j):
            copy.start()
    for copy in own_prompts:
        copy.start()
    pl.semaphore_wait(barrier, n - 1)

    def send_prompts(j):
        @pl.loop(1, n)
        def _(k):
            for i in range(2):
                prompt_copy(j, k, i).start()

    def send_window(j, condition):
        @pl.when(jnp.logical_and(chip < chips - 1, condition))
        def _():
            for copy in win_copies(j):
                copy.start()

    w_cross = remote(w, wst.at[0], w_send, w_recv, sibling)
    w_cross.start()
    send_prompts(0)
    send_window(0, core == 1)
    for j in range(half):
        for copy in cross_copies(j):
            copy.start()
        for copy in kv_cross(j):
            copy.start()

    acc[...] = jnp.zeros(acc.shape, jnp.float32)

    @pl.when(chip == 0)
    def _():
        kall[:, :, prompt : prompt + 2 * height] = jnp.zeros((half, 2, 2 * height, d), jnp.bfloat16)

    @pl.when(chip == chips - 1)
    def _():
        grecv[...] = jnp.zeros(grecv.shape, jnp.bfloat16)

    lens_local.wait()
    answers = lens.shape[1]
    row = lax.broadcasted_iota(jnp.int32, (answers, answers), 0)
    col = lax.broadcasted_iota(jnp.int32, (answers, answers), 1)
    starts = jnp.sum(
        jnp.where(col < row, jnp.broadcast_to(lst[...], (answers, answers)), 0),
        axis=1, keepdims=True,
    )
    key = lax.broadcasted_iota(jnp.int32, (height, height), 0)
    query = lax.broadcasted_iota(jnp.int32, (height, height), 1)
    tri = key <= query
    for b in range(2):
        base = (2 * chip + b) * height
        pos = base + lax.broadcasted_iota(jnp.int32, (1, height), 1)
        first = jnp.max(jnp.where(starts <= pos, starts, 0), axis=0, keepdims=True)
        bias[b, 0] = jnp.where(key + (base - height) >= first, 0.0, MASKED)
        both = jnp.where(tri, key + base, key + (base - 2 * height))
        bias[b, 1] = jnp.where(both >= first, 0.0, MASKED)
    tri_b[...] = tri.astype(jnp.float32).astype(jnp.bfloat16)

    def prepare(s, j):
        for h in range(group):
            rows = slice(h * height, (h + 1) * height)
            og_t = qog[s, j, 1, :, rows].T
            cots_t[s, j, :, rows] = (wst[s] * og_t.astype(jnp.float32)).astype(jnp.bfloat16)
            qs_t[s, j, :, rows] = qog[s, j, 0, :, rows].T

    w_local.wait()

    @pl.loop(0, half)
    def _(j):
        pltpu.make_async_copy(qog.at[1, j], qog.at[1, j], in_sem.at[j]).wait()
        prepare(1, j)

    send_window(0, core == 0)
    w_cross.wait_recv()

    @pl.loop(0, half)
    def _(j):
        pltpu.make_async_copy(qog.at[0, j], qog.at[0, j], xq_recv.at[j]).wait()
        prepare(0, j)

    for j in range(1, half):
        send_prompts(j)
    pltpu.make_async_copy(pgath.at[0], pgath.at[0], pg_recv.at[0]).wait()
    for j in range(1, half):
        send_window(j, True)

    def run_unit(j, b, leading):
        s = core if b == 1 else other
        if leading:
            mine = kall.at[j, :, block(2 + core)]
            pltpu.make_async_copy(mine, mine, kv_sem.at[j]).wait()
            theirs = kall.at[j, :, block(2 + other)]
            pltpu.make_async_copy(theirs, theirs, xk_recv.at[j]).wait()
            if j > 0:
                pltpu.make_async_copy(pgath.at[j], pgath.at[j], pg_recv.at[j]).wait()
            for i in range(2):
                gathered = pgath[j, i].astype(jnp.float32).reshape(prompt, d)
                kall[j, i, :prompt, :] = gathered.astype(jnp.bfloat16)

        needed = ((0,) if b == 0 else ()) + ((1,) if leading else ())

        @pl.when(chip > 0)
        def _():
            for t in needed:
                window = kall.at[j, :, block(t)]
                pltpu.make_async_copy(window, window, win_recv.at[j, t]).wait()

        near_far = slice(prompt + b * height, prompt + (b + 3) * height)
        tri2 = twice(tri)
        keys = jnp.concatenate([kall[j, 0, :prompt], kall[j, 0, near_far]], axis=0)
        values = jnp.concatenate([kall[j, 1, :prompt], kall[j, 1, near_far]], axis=0)
        vt[...] = values.T
        held = {}

        def rows_of(pair):
            return slice(pair * 2 * height, (pair + 1) * 2 * height)

        def score(pair):
            scores = dot(keys, qs_t[s, j, :, rows_of(pair)])
            s_p = scores[:at1]
            s_n = scores[at2:at3] + twice(bias[b, 0])
            s_c = jnp.where(tri2, scores[at3:], scores[at1:at2]) + twice(bias[b, 1])
            top = jnp.maximum(
                jnp.maximum(jnp.max(s_p, axis=0, keepdims=True), jnp.max(s_n, axis=0, keepdims=True)),
                jnp.max(s_c, axis=0, keepdims=True),
            )
            held[pair] = s_p, s_n, s_c, top

        def soften(pair):
            rows = rows_of(pair)
            s_p, s_n, s_c, top = held[pair]
            e_p = jnp.exp2((s_p - top) * log_factor)
            e_n = jnp.exp2((s_n - top) * log_factor)
            e_c = jnp.exp2((s_c - top) * log_factor)
            total = (
                jnp.sum(e_p, axis=0, keepdims=True)
                + jnp.sum(e_n, axis=0, keepdims=True)
                + jnp.sum(e_c, axis=0, keepdims=True)
            )
            p_all[s, j, :at1, rows] = e_p.astype(jnp.bfloat16)
            p_all[s, j, at2:at3, rows] = e_n.astype(jnp.bfloat16)
            b_c = e_c.astype(jnp.bfloat16)
            b_d = b_c * twice(tri_b[...])
            p_all[s, j, at1:at2, rows] = b_c - b_d
            p_all[s, j, at3:, rows] = b_d
            held[pair] = 1.0 / total

        def attend(pair):
            rows = rows_of(pair)
            inv = held[pair]
            out_t = (dot(vt[...], p_all[s, j, :, rows]) * inv).astype(jnp.bfloat16)
            cot_t = (cots_t[s, j, :, rows].astype(jnp.float32) * inv).astype(jnp.bfloat16)
            delta = jnp.sum(
                cot_t.astype(jnp.float32) * out_t.astype(jnp.float32), axis=0, keepdims=True
            )
            cots[s, j, rows, :] = cot_t.T
            out = out_t.T
            for h in range(2):
                lanes = slice((2 * pair + h) * d, (2 * pair + h + 1) * d)
                attn[s, j, :, lanes] = out[h * height : (h + 1) * height]
            held[pair] = cot_t, delta

        def slope(pair):
            rows = rows_of(pair)
            cot_t, delta = held[pair]
            slopes = dot(values, cot_t)
            ds_all[s, j, :, rows] = p_all[s, j, :, rows] * (slopes - delta).astype(jnp.bfloat16)

        pairs = group // 2
        for step in range(-2, pairs + 2):
            if 0 <= step < pairs:
                soften(step)
            if 0 <= step + 2 < pairs:
                score(step + 2)
            if 0 <= step - 1 < pairs:
                attend(step - 1)
            if 0 <= step - 2 < pairs:
                slope(step - 2)

        key_terms(j, b, slice(0, at3 if b == 0 else at2))

        @pl.when(s == 0)
        def _():
            out_copy(attn, j, at_send, at_recv).start()

    def key_terms(j, b, rows):
        s = core if b == 1 else other
        q_rows = jnp.concatenate([qog[s, j, 0, :, h * d : (h + 1) * d] for h in range(group)], axis=0)
        start = max(rows.start, at1)
        window = slice(start + b * height, rows.stop + b * height)
        for i in range(2):
            part = dot(ds_all[s, j, rows], q_rows) * factor if i == 0 else dot(p_all[s, j, rows], cots[s, j])
            if rows.start == 0:
                acc[j, i, :prompt] += part[:at1]
            acc[j, i, window] += part[start - rows.start :]

    for j in range(half):
        for place, b in enumerate((1, 0) if j == 0 else (0, 1)):
            run_unit(j, b, place == 0)
            if j > 0 and b == 0:
                send_back(j, 0)
        for i in range(2):
            psend[j, :, i] = acc[j, i, :prompt].reshape(n, own_prompt, d).astype(jnp.bfloat16)

        @pl.loop(1, n)
        def _(k):
            reduce_copy(j, k).start()

        pltpu.make_async_copy(psend.at[j, me], precv.at[core, j, chip], pr_recv.at[j]).start()
        if j == 0:
            send_back(j, 0)
        send_back(j, 1)

    @pl.loop(0, 2 * half)
    def _(u):
        s = u // half
        j = lax.rem(u, half)
        b = s * core + (1 - s) * other
        near_far = pl.ds(pl.multiple_of(prompt + b * height, height), 3 * height)
        kt[:, :at1] = kall[j, 0, :prompt].T
        kt[:, at1:] = kall[j, 0, near_far].T
        dq_t = (dot(kt[...], ds_all[s, j]) * factor).astype(jnp.bfloat16)
        for h in range(group):
            rows = slice(h * height, (h + 1) * height)
            dq[s, j, :, rows] = dq_t[:, rows].T

        @pl.when(s == 0)
        def _():
            out_copy(dq, j, dq_send, dq_recv).start()

    for j in range(half):
        key_terms(j, 0, slice(at3, at3 + height))
        key_terms(j, 1, slice(at2, at3 + height))
        sibling_copy(j).start()

    for j in range(half):
        sibling_copy(j).wait_recv()

        @pl.when(chip < chips - 1)
        def _():
            back = grecv.at[:, j]
            pltpu.make_async_copy(back, back, gr_recv.at[j]).wait()

        for i, grad in enumerate((akg, avg)):
            mine = acc[j, i, block(2 + core)] + grecv[core, j, i].astype(jnp.float32)
            grad[:, cols(core * half + j, d)] = mine.astype(jnp.bfloat16)
            mine = srecv[j, i] + grecv[other, j, i].astype(jnp.float32)
            grad[:, cols(other * half + j, d)] = mine.astype(jnp.bfloat16)
    for j in range(half):
        terms = precv.at[:, j]
        pltpu.make_async_copy(terms, terms, pr_recv.at[j]).wait()
        for t in range(2):
            lanes = slice((t * half + j) * d, (t * half + j + 1) * d)
            for i, grad in enumerate((pkg, pvg)):
                grad[:, lanes] = jnp.sum(precv[t, j, :, i].astype(jnp.float32), axis=0)

    w_cross.wait_send()
    for j in range(half):
        sent = pgath.at[j, :, pl.ds(0, n - 1)]
        pltpu.make_async_copy(sent, sent, pg_send.at[j]).wait()
        pltpu.make_async_copy(qog.at[1, j], qog.at[1, j], xq_send.at[j]).wait()
        mine = kall.at[j, :, block(2 + core)]
        pltpu.make_async_copy(mine, mine, xk_send.at[j]).wait()

        @pl.when(chip < chips - 1)
        def _():
            window = kall.at[j, :, pl.ds(prompt, 2 * height)]
            pltpu.make_async_copy(window, window, win_send.at[j]).wait()

        @pl.when(chip > 0)
        def _():
            for t in range(2):
                back_copy(j, t).wait_send()

        sent = psend.at[j, pl.ds(0, n - 1)]
        pltpu.make_async_copy(sent, sent, pr_send.at[j]).wait()
        sibling_copy(j).wait_send()
        out_copy(attn, j, at_send, at_recv).wait()
        out_copy(dq, j, dq_send, dq_recv).wait()


def write_out(kv_heads, span, attn, dq, akg, avg, pkg, pvg, *refs):
    outs, (wide_sem, sem) = refs[:6], refs[6:]
    half = kv_heads // 2
    core = lax.rem(lax.axis_index("row"), 2)
    copies = [
        pltpu.make_async_copy(
            v.at[1 + t, j],
            out.at[:, pl.ds(pl.multiple_of((jnp.abs(core - t) * half + j) * span, span), span)],
            wide_sem.at[i, t, j],
        )
        for i, (v, out) in enumerate(((attn, outs[0]), (dq, outs[1])))
        for t in range(2)
        for j in range(half)
    ] + [
        pltpu.make_async_copy(v, out, sem.at[i])
        for i, (v, out) in enumerate(zip((akg, avg, pkg, pvg), outs[2:]))
    ]
    for copy in copies:
        copy.start()
    for copy in copies:
        copy.wait()


def per_device(n, queries, answer_keys, answer_values, prompt_keys, prompt_values, out_grad, weights, lengths):
    height = queries.shape[0]
    d = HEAD_DIM
    columns = answer_keys.shape[1]
    kv_heads = columns // d
    half = kv_heads // 2
    chips = n // 2
    group = queries.shape[1] // columns
    own_prompt = prompt_keys.shape[0]
    keys = own_prompt * n + 3 * height
    held = own_prompt * n + 4 * height
    span = group * d
    answers = lengths.shape[0]
    bf16, f32 = jnp.bfloat16, jnp.float32
    vmem = pl.BlockSpec(memory_space=pltpu.VMEM)
    hbm = pl.BlockSpec(memory_space=pltpu.HBM)
    dma = pltpu.SemaphoreType.DMA
    results = pl.pallas_call(
        functools.partial(kernel, n, kv_heads, group),
        out_shape=(
            pltpu.VMEM((3, half, height, span), bf16),
            pltpu.VMEM((3, half, height, span), bf16),
            pltpu.VMEM(answer_keys.shape, bf16),
            pltpu.VMEM(answer_keys.shape, bf16),
            pltpu.VMEM(prompt_keys.shape, f32),
            pltpu.VMEM(prompt_keys.shape, f32),
        ),
        in_specs=[hbm] * 8,
        out_specs=(vmem,) * 6,
        scratch_shapes=[
            pltpu.VMEM((2, half, 2, height, span), bf16),
            pltpu.VMEM((half, 2, held, d), bf16),
            pltpu.VMEM((d, keys), bf16),
            pltpu.VMEM((d, keys), bf16),
            pltpu.VMEM((half, 2, n, own_prompt, d), bf16),
            pltpu.VMEM((2, 1, height), f32),
            pltpu.VMEM((1, answers), jnp.int32),
            pltpu.VMEM((2, half, d, group * height), bf16),
            pltpu.VMEM((2, half, group * height, d), bf16),
            pltpu.VMEM((2, half, d, group * height), bf16),
            pltpu.VMEM((2, half, keys, group * height), bf16),
            pltpu.VMEM((2, half, keys, group * height), bf16),
            pltpu.VMEM((half, 2, held, d), f32),
            pltpu.VMEM((half, n, 2, own_prompt, d), bf16),
            pltpu.VMEM((2, half, chips, 2, own_prompt, d), bf16),
            pltpu.VMEM((half, 2, 2, height, d), bf16),
            pltpu.VMEM((2, half, 2, height, d), bf16),
            pltpu.VMEM((half, 2, height, d), f32),
            pltpu.VMEM((2, 2, height, height), f32),
            pltpu.VMEM((height, height), bf16),
            dma((2,)),
            dma((half,)), dma((half,)), dma((half,)), dma((half,)),
            dma((half, 2)),
            *[dma((half,))] * 11,
            dma((half, 2)),
            *[dma((half,))] * 3,
            dma, dma,
        ],
        compiler_params=pltpu.CompilerParams(
            collective_id=0, has_side_effects=True, vmem_limit_bytes=60 * 1024 * 1024
        ),
    )(
        queries, out_grad, answer_keys, answer_values, prompt_keys, prompt_values,
        weights.reshape(1, height), lengths.reshape(1, answers),
    )
    return pl.pallas_call(
        functools.partial(write_out, kv_heads, span),
        out_shape=(
            jax.ShapeDtypeStruct(queries.shape, bf16),
            jax.ShapeDtypeStruct(queries.shape, bf16),
            jax.ShapeDtypeStruct(answer_keys.shape, bf16),
            jax.ShapeDtypeStruct(answer_keys.shape, bf16),
            jax.ShapeDtypeStruct(prompt_keys.shape, f32),
            jax.ShapeDtypeStruct(prompt_keys.shape, f32),
        ),
        in_specs=[vmem] * 6,
        out_specs=(hbm,) * 6,
        scratch_shapes=[dma((2, 2, half)), dma((4,))],
        compiler_params=pltpu.CompilerParams(vmem_limit_bytes=8 * 1024 * 1024),
    )(*results)


def solution(mesh):
    both = ("grp", "row")
    wide = P(both, None)
    return jax.shard_map(
        functools.partial(per_device, mesh.shape["row"]),
        mesh=mesh,
        in_specs=(wide,) * 6 + (P(both), P("grp")),
        out_specs=(wide,) * 6,
        check_vma=False,
    )
```

```python
import functools
import math

import jax
import jax.numpy as jnp
from jax import lax
from jax.experimental import pallas as pl
from jax.experimental.pallas import tpu as pltpu
from jax.sharding import PartitionSpec as P

HEAD_DIM = 128
MASKED = -1e30
MESH = pl.DeviceIdType.MESH


def dot(a, b):
    return jnp.dot(a, b, preferred_element_type=jnp.float32)


def twice(x):
    return jnp.concatenate([x, x], axis=1)


def kernel(
    n, kv_heads, group,
    q_hbm, og_hbm, ak, av, pk, pv, w, lens,
    attn, dq, akg, avg, pkg, pvg,
    qog, kall, vt, kt, pgath, wst, lst, qs_t, cots, cots_t, p_all, ds_all, acc,
    psend, precv, gsend, grecv, srecv, bias, tri_b,
    small_sem, in_sem, kv_sem, xq_recv, xk_recv, win_recv, pg_recv, pr_recv, gr_recv, sr_recv, at_recv, dq_recv,
    xq_send, xk_send, win_send, pg_send, pr_send, gs_send, sr_send, at_send, dq_send, w_recv, w_send,
):
    me = lax.axis_index("row")
    height = ak.shape[0]
    d = HEAD_DIM
    span = group * d
    half = kv_heads // 2
    own_prompt = pk.shape[0]
    prompt = own_prompt * n
    factor = d ** (-0.5)
    log_factor = factor * math.log2(math.e)
    chips = n // 2
    core = lax.rem(me, 2)
    other = 1 - core
    chip = me // 2
    sibling = me + 1 - 2 * core
    after = lax.rem(chip + 1, chips)
    before = lax.rem(chip + chips - 1, chips)
    at1, at2, at3 = prompt, prompt + height, prompt + 2 * height

    def remote(src, dst, send, recv, target):
        return pltpu.make_async_remote_copy(
            src_ref=src, dst_ref=dst, send_sem=send, recv_sem=recv,
            device_id={"row": target}, device_id_type=MESH,
        )

    def cols(at, width):
        return pl.ds(pl.multiple_of(at * width, width), width)

    def block(b):
        return pl.ds(pl.multiple_of(prompt + b * height, height), height)

    def in_copies(j):
        head = core * half + j
        return (
            pltpu.make_async_copy(q_hbm.at[:, cols(head, span)], qog.at[1, j, 0], in_sem.at[j]),
            pltpu.make_async_copy(og_hbm.at[:, cols(head, span)], qog.at[1, j, 1], in_sem.at[j]),
        )

    def cross_copies(j):
        head = other * half + j
        return (
            remote(og_hbm.at[:, cols(head, span)], qog.at[0, j, 1], xq_send.at[j], xq_recv.at[j], sibling),
            remote(q_hbm.at[:, cols(head, span)], qog.at[0, j, 0], xq_send.at[j], xq_recv.at[j], sibling),
        )

    def kv_copies(j):
        head = core * half + j
        return [
            pltpu.make_async_copy(src.at[:, cols(head, d)], kall.at[j, i, block(2 + core)], kv_sem.at[j])
            for i, src in enumerate((ak, av))
        ]

    def kv_cross(j):
        head = other * half + j
        return [
            remote(src.at[:, cols(head, d)], kall.at[j, i, block(2 + core)], xk_send.at[j], xk_recv.at[j], sibling)
            for i, src in enumerate((ak, av))
        ]

    def win_copy(j, i, t):
        return remote(
            (ak, av)[i].at[:, pl.ds((t * half + j) * d, d)], kall.at[j, i, block(core)],
            win_send.at[j], win_recv.at[j, core, i], 2 * after + t,
        )

    def prompt_copy(j, k, i):
        target = lax.rem(me + k, n)
        return remote(
            (pk, pv)[i].at[:, cols(lax.rem(target, 2) * half + j, d)], pgath.at[j, i, me],
            pg_send.at[j], pg_recv.at[j, i], target,
        )

    def reduce_copy(j, k, part):
        target = lax.rem(me + k, n)
        return remote(
            psend.at[j, part, target], precv.at[core, j, part, chip], pr_send.at[j], pr_recv.at[j], target
        )

    def send_reduce(j, part):
        for i in range(part.start, part.start + part.size):
            psend[j, i] = acc[j, i, :prompt].reshape(n, own_prompt, d).astype(jnp.bfloat16)

        @pl.loop(1, n)
        def _(k):
            reduce_copy(j, k, part).start()

        pltpu.make_async_copy(psend.at[j, part, me], precv.at[core, j, part, chip], pr_recv.at[j]).start()

    def back_copy(j, t, part):
        return remote(
            gsend.at[j, t, part], grecv.at[core, j, part], gs_send.at[j, t], gr_recv.at[j], 2 * before + t
        )

    def send_back(j, t, part):
        for i in range(part.start, part.start + part.size):
            gsend[j, t, i] = acc[j, i, prompt + t * height : prompt + (t + 1) * height].astype(jnp.bfloat16)

        @pl.when(chip > 0)
        def _():
            back_copy(j, t, part).start()

    def sibling_copy(j):
        return remote(acc.at[j, :, block(2 + other)], srecv.at[j], sr_send.at[j], sr_recv.at[j], sibling)

    def out_copy(ref, j, send, recv):
        return remote(ref.at[0, j], ref.at[2, j], send.at[j], recv.at[j], sibling)

    barrier = pltpu.get_barrier_semaphore()

    @pl.loop(1, n)
    def _(k):
        pl.semaphore_signal(barrier, inc=1, device_id={"row": lax.rem(me + k, n)}, device_id_type=MESH)

    w_local = pltpu.make_async_copy(w, wst.at[1], small_sem.at[0])
    lens_local = pltpu.make_async_copy(lens, lst, small_sem.at[1])
    own_prompts = [
        pltpu.make_async_copy((pk, pv)[i].at[:, cols(core * half + j, d)], pgath.at[j, i, me], pg_recv.at[j, i])
        for j in range(half)
        for i in range(2)
    ]
    w_local.start()
    lens_local.start()
    for j in range(half):
        for copy in in_copies(j):
            copy.start()
    for j in range(half):
        for copy in kv_copies(j):
            copy.start()
    for copy in own_prompts:
        copy.start()
    pl.semaphore_wait(barrier, n - 1)

    def send_prompts(j, i):
        @pl.loop(1, n)
        def _(k):
            prompt_copy(j, k, i).start()

    def send_window(j, i, condition):
        @pl.when(jnp.logical_and(chip < chips - 1, condition))
        def _():
            for t in range(2):
                win_copy(j, i, t).start()

    w_cross = remote(w, wst.at[0], w_send, w_recv, sibling)
    w_cross.start()
    for i in range(2):
        send_prompts(0, i)
        send_window(0, i, core == 1)
    for j in range(half):
        for copy in cross_copies(j):
            copy.start()
        for copy in kv_cross(j):
            copy.start()

    acc[...] = jnp.zeros(acc.shape, jnp.float32)

    @pl.when(chip == 0)
    def _():
        kall[:, :, prompt : prompt + 2 * height] = jnp.zeros((half, 2, 2 * height, d), jnp.bfloat16)

    @pl.when(chip == chips - 1)
    def _():
        grecv[...] = jnp.zeros(grecv.shape, jnp.bfloat16)

    lens_local.wait()
    answers = lens.shape[1]
    row = lax.broadcasted_iota(jnp.int32, (answers, answers), 0)
    col = lax.broadcasted_iota(jnp.int32, (answers, answers), 1)
    starts = jnp.sum(
        jnp.where(col < row, jnp.broadcast_to(lst[...], (answers, answers)), 0),
        axis=1, keepdims=True,
    )
    key = lax.broadcasted_iota(jnp.int32, (height, height), 0)
    query = lax.broadcasted_iota(jnp.int32, (height, height), 1)
    tri = key <= query
    for b in range(2):
        base = (2 * chip + b) * height
        pos = base + lax.broadcasted_iota(jnp.int32, (1, height), 1)
        first = jnp.max(jnp.where(starts <= pos, starts, 0), axis=0, keepdims=True)
        bias[b, 0] = jnp.where(key + (base - height) >= first, 0.0, MASKED)
        both = jnp.where(tri, key + base, key + (base - 2 * height))
        bias[b, 1] = jnp.where(both >= first, 0.0, MASKED)
    tri_b[...] = tri.astype(jnp.float32).astype(jnp.bfloat16)

    def prepare(s, j):
        for h in range(group):
            rows = slice(h * height, (h + 1) * height)
            og_t = qog[s, j, 1, :, rows].T
            cots_t[s, j, :, rows] = (wst[s] * og_t.astype(jnp.float32)).astype(jnp.bfloat16)
            qs_t[s, j, :, rows] = qog[s, j, 0, :, rows].T

    w_local.wait()

    @pl.loop(0, half)
    def _(j):
        pltpu.make_async_copy(qog.at[1, j], qog.at[1, j], in_sem.at[j]).wait()
        prepare(1, j)

    for i in range(2):
        send_window(0, i, core == 0)
    w_cross.wait_recv()

    @pl.loop(0, half)
    def _(j):
        pltpu.make_async_copy(qog.at[0, j], qog.at[0, j], xq_recv.at[j]).wait()
        prepare(0, j)

    for j in range(1, half):
        for i in range(2):
            send_prompts(j, i)
    pltpu.make_async_copy(pgath.at[0, 0], pgath.at[0, 0], pg_recv.at[0, 0]).wait()
    for j in range(1, half):
        for i in range(2):
            send_window(j, i, True)

    def assemble(j, i):
        if j > 0 or i > 0:
            pltpu.make_async_copy(pgath.at[j, i], pgath.at[j, i], pg_recv.at[j, i]).wait()
        gathered = pgath[j, i].astype(jnp.float32).reshape(prompt, d)
        kall[j, i, :prompt, :] = gathered.astype(jnp.bfloat16)

    def arrive(j, i, b, leading):
        if leading:
            assemble(j, i)

        @pl.when(chip > 0)
        def _():
            for t in ((0,) if b == 0 else ()) + ((1,) if leading else ()):
                window = kall.at[j, i, block(t)]
                pltpu.make_async_copy(window, window, win_recv.at[j, t, i]).wait()

    def run_unit(j, b, leading):
        s = core if b == 1 else other
        if leading:
            mine = kall.at[j, :, block(2 + core)]
            pltpu.make_async_copy(mine, mine, kv_sem.at[j]).wait()
            theirs = kall.at[j, :, block(2 + other)]
            pltpu.make_async_copy(theirs, theirs, xk_recv.at[j]).wait()
        arrive(j, 0, b, leading)
        late = leading and j == 0
        if not late:
            arrive(j, 1, b, leading)

        near_far = slice(prompt + b * height, prompt + (b + 3) * height)
        tri2 = twice(tri)
        keys = jnp.concatenate([kall[j, 0, :prompt], kall[j, 0, near_far]], axis=0)

        def values():
            return jnp.concatenate([kall[j, 1, :prompt], kall[j, 1, near_far]], axis=0)

        if not late:
            vt[...] = values().T
        held = {}

        def rows_of(pair):
            return slice(pair * 2 * height, (pair + 1) * 2 * height)

        def score(pair):
            scores = dot(keys, qs_t[s, j, :, rows_of(pair)])
            s_p = scores[:at1]
            s_n = scores[at2:at3] + twice(bias[b, 0])
            s_c = jnp.where(tri2, scores[at3:], scores[at1:at2]) + twice(bias[b, 1])
            top = jnp.maximum(
                jnp.maximum(jnp.max(s_p, axis=0, keepdims=True), jnp.max(s_n, axis=0, keepdims=True)),
                jnp.max(s_c, axis=0, keepdims=True),
            )
            held[pair] = s_p, s_n, s_c, top

        def soften(pair):
            rows = rows_of(pair)
            s_p, s_n, s_c, top = held[pair]
            e_p = jnp.exp2((s_p - top) * log_factor)
            e_n = jnp.exp2((s_n - top) * log_factor)
            e_c = jnp.exp2((s_c - top) * log_factor)
            total = (
                jnp.sum(e_p, axis=0, keepdims=True)
                + jnp.sum(e_n, axis=0, keepdims=True)
                + jnp.sum(e_c, axis=0, keepdims=True)
            )
            p_all[s, j, :at1, rows] = e_p.astype(jnp.bfloat16)
            p_all[s, j, at2:at3, rows] = e_n.astype(jnp.bfloat16)
            b_c = e_c.astype(jnp.bfloat16)
            b_d = b_c * twice(tri_b[...])
            p_all[s, j, at1:at2, rows] = b_c - b_d
            p_all[s, j, at3:, rows] = b_d
            held[pair] = 1.0 / total

        def attend(pair):
            rows = rows_of(pair)
            inv = held[pair]
            out_t = (dot(vt[...], p_all[s, j, :, rows]) * inv).astype(jnp.bfloat16)
            cot_t = (cots_t[s, j, :, rows].astype(jnp.float32) * inv).astype(jnp.bfloat16)
            delta = jnp.sum(
                cot_t.astype(jnp.float32) * out_t.astype(jnp.float32), axis=0, keepdims=True
            )
            cots[s, j, rows, :] = cot_t.T
            out = out_t.T
            for h in range(2):
                lanes = slice((2 * pair + h) * d, (2 * pair + h + 1) * d)
                attn[s, j, :, lanes] = out[h * height : (h + 1) * height]
            held[pair] = cot_t, delta

        def slope(pair):
            rows = rows_of(pair)
            cot_t, delta = held[pair]
            slopes = dot(values(), cot_t)
            ds_all[s, j, :, rows] = p_all[s, j, :, rows] * (slopes - delta).astype(jnp.bfloat16)

        pairs = group // 2
        rows = slice(0, at3 if b == 0 else at2)
        for step in range(-2, pairs + 2):
            if 0 <= step < pairs:
                soften(step)
            if 0 <= step + 2 < pairs:
                score(step + 2)
            if late and step == 0:
                arrive(j, 1, b, leading)
                vt[...] = values().T
            if 0 <= step - 1 < pairs:
                attend(step - 1)
            if 0 <= step - 2 < pairs:
                slope(step - 2)

        key_terms(j, b, 0, rows)
        key_terms(j, b, 1, rows)
        @pl.when(s == 0)
        def _():
            out_copy(attn, j, at_send, at_recv).start()

    def key_terms(j, b, i, rows):
        s = core if b == 1 else other
        start = max(rows.start, at1)
        window = slice(start + b * height, rows.stop + b * height)
        if i == 0:
            q_rows = jnp.concatenate([qog[s, j, 0, :, h * d : (h + 1) * d] for h in range(group)], axis=0)
            part = dot(ds_all[s, j, rows], q_rows) * factor
        else:
            part = dot(p_all[s, j, rows], cots[s, j])
        if rows.start == 0:
            acc[j, i, :prompt] += part[:at1]
        acc[j, i, window] += part[start - rows.start :]

    for j in range(half):
        for place, b in enumerate((1, 0) if j == 0 else (0, 1)):
            run_unit(j, b, place == 0)
            if j > 0 and b == 0:
                send_back(j, 0, pl.ds(0, 2))
        send_reduce(j, pl.ds(0, 2))
        if j == 0:
            send_back(j, 0, pl.ds(0, 2))
        send_back(j, 1, pl.ds(0, 2))

    @pl.loop(0, 2 * half)
    def _(u):
        s = u // half
        j = lax.rem(u, half)
        b = s * core + (1 - s) * other
        near_far = pl.ds(pl.multiple_of(prompt + b * height, height), 3 * height)
        kt[:, :at1] = kall[j, 0, :prompt].T
        kt[:, at1:] = kall[j, 0, near_far].T
        dq_t = (dot(kt[...], ds_all[s, j]) * factor).astype(jnp.bfloat16)
        for h in range(group):
            rows = slice(h * height, (h + 1) * height)
            dq[s, j, :, rows] = dq_t[:, rows].T

        @pl.when(s == 0)
        def _():
            out_copy(dq, j, dq_send, dq_recv).start()

    for j in range(half):
        for i in range(2):
            key_terms(j, 0, i, slice(at3, at3 + height))
            key_terms(j, 1, i, slice(at2, at3 + height))
        sibling_copy(j).start()

    for j in range(half):
        sibling_copy(j).wait_recv()

        @pl.when(chip < chips - 1)
        def _():
            back = grecv.at[:, j]
            pltpu.make_async_copy(back, back, gr_recv.at[j]).wait()

        for i, grad in enumerate((akg, avg)):
            mine = acc[j, i, block(2 + core)] + grecv[core, j, i].astype(jnp.float32)
            grad[:, cols(core * half + j, d)] = mine.astype(jnp.bfloat16)
            mine = srecv[j, i] + grecv[other, j, i].astype(jnp.float32)
            grad[:, cols(other * half + j, d)] = mine.astype(jnp.bfloat16)
    for j in range(half):
        terms = precv.at[:, j]
        pltpu.make_async_copy(terms, terms, pr_recv.at[j]).wait()
        for t in range(2):
            lanes = slice((t * half + j) * d, (t * half + j + 1) * d)
            for i, grad in enumerate((pkg, pvg)):
                grad[:, lanes] = jnp.sum(precv[t, j, i].astype(jnp.float32), axis=0)

    w_cross.wait_send()
    for j in range(half):
        sent = pgath.at[j, :, pl.ds(0, n - 1)]
        pltpu.make_async_copy(sent, sent, pg_send.at[j]).wait()
        pltpu.make_async_copy(qog.at[1, j], qog.at[1, j], xq_send.at[j]).wait()
        mine = kall.at[j, :, block(2 + core)]
        pltpu.make_async_copy(mine, mine, xk_send.at[j]).wait()

        @pl.when(chip < chips - 1)
        def _():
            window = kall.at[j, :, pl.ds(prompt, 2 * height)]
            pltpu.make_async_copy(window, window, win_send.at[j]).wait()

        @pl.when(chip > 0)
        def _():
            for t in range(2):
                back_copy(j, t, pl.ds(0, 2)).wait_send()

        sent = psend.at[j, :, pl.ds(0, n - 1)]
        pltpu.make_async_copy(sent, sent, pr_send.at[j]).wait()
        sibling_copy(j).wait_send()
        out_copy(attn, j, at_send, at_recv).wait()
        out_copy(dq, j, dq_send, dq_recv).wait()


def write_out(kv_heads, span, attn, dq, akg, avg, pkg, pvg, *refs):
    outs, (wide_sem, sem) = refs[:6], refs[6:]
    half = kv_heads // 2
    core = lax.rem(lax.axis_index("row"), 2)
    copies = [
        pltpu.make_async_copy(
            v.at[1 + t, j],
            out.at[:, pl.ds(pl.multiple_of((jnp.abs(core - t) * half + j) * span, span), span)],
            wide_sem.at[i, t, j],
        )
        for i, (v, out) in enumerate(((attn, outs[0]), (dq, outs[1])))
        for t in range(2)
        for j in range(half)
    ] + [
        pltpu.make_async_copy(v, out, sem.at[i])
        for i, (v, out) in enumerate(zip((akg, avg, pkg, pvg), outs[2:]))
    ]
    for copy in copies:
        copy.start()
    for copy in copies:
        copy.wait()


def per_device(n, queries, answer_keys, answer_values, prompt_keys, prompt_values, out_grad, weights, lengths):
    height = queries.shape[0]
    d = HEAD_DIM
    columns = answer_keys.shape[1]
    kv_heads = columns // d
    half = kv_heads // 2
    chips = n // 2
    group = queries.shape[1] // columns
    own_prompt = prompt_keys.shape[0]
    keys = own_prompt * n + 3 * height
    held = own_prompt * n + 4 * height
    span = group * d
    answers = lengths.shape[0]
    bf16, f32 = jnp.bfloat16, jnp.float32
    vmem = pl.BlockSpec(memory_space=pltpu.VMEM)
    hbm = pl.BlockSpec(memory_space=pltpu.HBM)
    dma = pltpu.SemaphoreType.DMA
    results = pl.pallas_call(
        functools.partial(kernel, n, kv_heads, group),
        out_shape=(
            pltpu.VMEM((3, half, height, span), bf16),
            pltpu.VMEM((3, half, height, span), bf16),
            pltpu.VMEM(answer_keys.shape, bf16),
            pltpu.VMEM(answer_keys.shape, bf16),
            pltpu.VMEM(prompt_keys.shape, f32),
            pltpu.VMEM(prompt_keys.shape, f32),
        ),
        in_specs=[hbm] * 8,
        out_specs=(vmem,) * 6,
        scratch_shapes=[
            pltpu.VMEM((2, half, 2, height, span), bf16),
            pltpu.VMEM((half, 2, held, d), bf16),
            pltpu.VMEM((d, keys), bf16),
            pltpu.VMEM((d, keys), bf16),
            pltpu.VMEM((half, 2, n, own_prompt, d), bf16),
            pltpu.VMEM((2, 1, height), f32),
            pltpu.VMEM((1, answers), jnp.int32),
            pltpu.VMEM((2, half, d, group * height), bf16),
            pltpu.VMEM((2, half, group * height, d), bf16),
            pltpu.VMEM((2, half, d, group * height), bf16),
            pltpu.VMEM((2, half, keys, group * height), bf16),
            pltpu.VMEM((2, half, keys, group * height), bf16),
            pltpu.VMEM((half, 2, held, d), f32),
            pltpu.VMEM((half, 2, n, own_prompt, d), bf16),
            pltpu.VMEM((2, half, 2, chips, own_prompt, d), bf16),
            pltpu.VMEM((half, 2, 2, height, d), bf16),
            pltpu.VMEM((2, half, 2, height, d), bf16),
            pltpu.VMEM((half, 2, height, d), f32),
            pltpu.VMEM((2, 2, height, height), f32),
            pltpu.VMEM((height, height), bf16),
            dma((2,)),
            dma((half,)), dma((half,)), dma((half,)), dma((half,)),
            dma((half, 2, 2)),
            dma((half, 2)),
            *[dma((half,))] * 10,
            dma((half, 2)),
            *[dma((half,))] * 3,
            dma, dma,
        ],
        compiler_params=pltpu.CompilerParams(
            collective_id=0, has_side_effects=True, vmem_limit_bytes=60 * 1024 * 1024
        ),
    )(
        queries, out_grad, answer_keys, answer_values, prompt_keys, prompt_values,
        weights.reshape(1, height), lengths.reshape(1, answers),
    )
    return pl.pallas_call(
        functools.partial(write_out, kv_heads, span),
        out_shape=(
            jax.ShapeDtypeStruct(queries.shape, bf16),
            jax.ShapeDtypeStruct(queries.shape, bf16),
            jax.ShapeDtypeStruct(answer_keys.shape, bf16),
            jax.ShapeDtypeStruct(answer_keys.shape, bf16),
            jax.ShapeDtypeStruct(prompt_keys.shape, f32),
            jax.ShapeDtypeStruct(prompt_keys.shape, f32),
        ),
        in_specs=[vmem] * 6,
        out_specs=(hbm,) * 6,
        scratch_shapes=[dma((2, 2, half)), dma((4,))],
        compiler_params=pltpu.CompilerParams(vmem_limit_bytes=8 * 1024 * 1024),
    )(*results)


def solution(mesh):
    both = ("grp", "row")
    wide = P(both, None)
    return jax.shard_map(
        functools.partial(per_device, mesh.shape["row"]),
        mesh=mesh,
        in_specs=(wide,) * 6 + (P(both), P("grp")),
        out_specs=(wide,) * 6,
        check_vma=False,
    )
```

```python
import functools
import math

import jax
import jax.numpy as jnp
from jax import lax
from jax.experimental import pallas as pl
from jax.experimental.pallas import tpu as pltpu
from jax.sharding import PartitionSpec as P

HEAD_DIM = 128
MASKED = -1e30
MESH = pl.DeviceIdType.MESH


def dot(a, b):
    return jnp.dot(a, b, preferred_element_type=jnp.float32)


def twice(x):
    return jnp.concatenate([x, x], axis=1)


def kernel(
    n, kv_heads, group,
    q_hbm, og_hbm, ak, av, pk, pv, w, lens,
    attn, dq, akg, avg, pkg, pvg,
    qog, kall, vt, kt, pgath, wst, lst, qs_t, cots, cots_t, p_all, ds_all, acc,
    psend, precv, gsend, grecv, srecv, bias, tri_b, deltas,
    small_sem, in_sem, kv_sem, xq_recv, xk_recv, win_recv, pg_recv, pr_recv, gr_recv, sr_recv, at_recv, dq_recv,
    xq_send, xk_send, win_send, pg_send, pr_send, gs_send, sr_send, at_send, dq_send, w_recv, w_send, go,
):
    me = lax.axis_index("row")
    height = ak.shape[0]
    d = HEAD_DIM
    span = group * d
    half = kv_heads // 2
    own_prompt = pk.shape[0]
    prompt = own_prompt * n
    factor = d ** (-0.5)
    log_factor = factor * math.log2(math.e)
    chips = n // 2
    core = lax.rem(me, 2)
    other = 1 - core
    chip = me // 2
    sibling = me + 1 - 2 * core
    after = lax.rem(chip + 1, chips)
    before = lax.rem(chip + chips - 1, chips)
    at1, at2, at3 = prompt, prompt + height, prompt + 2 * height

    def remote(src, dst, send, recv, target):
        return pltpu.make_async_remote_copy(
            src_ref=src, dst_ref=dst, send_sem=send, recv_sem=recv,
            device_id={"row": target}, device_id_type=MESH,
        )

    def cols(at, width):
        return pl.ds(pl.multiple_of(at * width, width), width)

    def block(b):
        return pl.ds(pl.multiple_of(prompt + b * height, height), height)

    def in_copies(j):
        head = core * half + j
        return (
            pltpu.make_async_copy(q_hbm.at[:, cols(head, span)], qog.at[1, j, 0], in_sem.at[j]),
            pltpu.make_async_copy(og_hbm.at[:, cols(head, span)], qog.at[1, j, 1], in_sem.at[j]),
        )

    def cross_copies(j):
        head = other * half + j
        return (
            remote(og_hbm.at[:, cols(head, span)], qog.at[0, j, 1], xq_send.at[j], xq_recv.at[j], sibling),
            remote(q_hbm.at[:, cols(head, span)], qog.at[0, j, 0], xq_send.at[j], xq_recv.at[j], sibling),
        )

    def kv_copies(j):
        head = core * half + j
        return [
            pltpu.make_async_copy(src.at[:, cols(head, d)], kall.at[j, i, block(2 + core)], kv_sem.at[j])
            for i, src in enumerate((ak, av))
        ]

    def kv_cross(j):
        head = other * half + j
        return [
            remote(src.at[:, cols(head, d)], kall.at[j, i, block(2 + core)], xk_send.at[j], xk_recv.at[j], sibling)
            for i, src in enumerate((ak, av))
        ]

    def win_copy(j, i, t):
        return remote(
            (ak, av)[i].at[:, pl.ds((t * half + j) * d, d)], kall.at[j, i, block(core)],
            win_send.at[j], win_recv.at[j, core, i], 2 * after + t,
        )

    def prompt_copy(j, k, i):
        target = lax.rem(me + k, n)
        return remote(
            (pk, pv)[i].at[:, cols(lax.rem(target, 2) * half + j, d)], pgath.at[j, i, me],
            pg_send.at[j], pg_recv.at[j, i], target,
        )

    def reduce_copy(j, k, part):
        target = lax.rem(me + k, n)
        return remote(
            psend.at[j, part, target], precv.at[core, j, part, chip], pr_send.at[j], pr_recv.at[j], target
        )

    def send_reduce(j, part):
        for i in range(part.start, part.start + part.size):
            psend[j, i] = acc[j, i, :prompt].reshape(n, own_prompt, d).astype(jnp.bfloat16)

        @pl.loop(1, n)
        def _(k):
            reduce_copy(j, k, part).start()

        pltpu.make_async_copy(psend.at[j, part, me], precv.at[core, j, part, chip], pr_recv.at[j]).start()

    def back_copy(j, t, part):
        return remote(
            gsend.at[j, t, part], grecv.at[core, j, part], gs_send.at[j, t], gr_recv.at[j], 2 * before + t
        )

    def send_back(j, t, part):
        for i in range(part.start, part.start + part.size):
            gsend[j, t, i] = acc[j, i, prompt + t * height : prompt + (t + 1) * height].astype(jnp.bfloat16)

        @pl.when(chip > 0)
        def _():
            back_copy(j, t, part).start()

    def sibling_copy(j):
        return remote(acc.at[j, :, block(2 + other)], srecv.at[j], sr_send.at[j], sr_recv.at[j], sibling)

    def out_copy(ref, j, send, recv):
        return remote(ref.at[0, j], ref.at[2, j], send.at[j], recv.at[j], sibling)

    barrier = pltpu.get_barrier_semaphore()

    def signal(semaphore, target):
        pl.semaphore_signal(semaphore, inc=1, device_id={"row": target}, device_id_type=MESH)

    collector = n - 2

    @pl.when(me < n - 4)
    def _():
        signal(barrier, collector)

    @pl.when(chip > 0)
    def _():
        for t in range(2):
            signal(barrier, 2 * before + t)

    @pl.when(chip < chips - 1)
    def _():
        for t in range(2):
            signal(barrier, 2 * after + t)

    signal(barrier, sibling)

    w_local = pltpu.make_async_copy(w, wst.at[1], small_sem.at[0])
    lens_local = pltpu.make_async_copy(lens, lst, small_sem.at[1])
    own_prompts = [
        pltpu.make_async_copy((pk, pv)[i].at[:, cols(core * half + j, d)], pgath.at[j, i, me], pg_recv.at[j, i])
        for j in range(half)
        for i in range(2)
    ]
    w_local.start()
    lens_local.start()
    for j in range(half):
        for copy in in_copies(j):
            copy.start()
    for j in range(half):
        for copy in kv_copies(j):
            copy.start()
    for copy in own_prompts:
        copy.start()
    @pl.when(me == collector)
    def _():
        pl.semaphore_wait(barrier, n - 1)

        @pl.loop(1, n)
        def _(k):
            signal(go, lax.rem(me + k, n))

    @pl.when(me != collector)
    def _():
        pl.semaphore_wait(
            barrier, 1 + 2 * (chip > 0).astype(jnp.int32) + 2 * (chip < chips - 1).astype(jnp.int32)
        )


    def send_prompts(j, i):
        @pl.loop(1, n)
        def _(k):
            prompt_copy(j, k, i).start()

    def send_window(j, i, condition):
        @pl.when(jnp.logical_and(chip < chips - 1, condition))
        def _():
            for t in range(2):
                win_copy(j, i, t).start()

    w_cross = remote(w, wst.at[0], w_send, w_recv, sibling)
    w_cross.start()
    for i in range(2):
        send_window(0, i, core == 1)
    send_window(0, 0, core == 0)
    for j in range(half):
        for copy in cross_copies(j):
            copy.start()
        for copy in kv_cross(j):
            copy.start()

    @pl.when(me != collector)
    def _():
        pl.semaphore_wait(go, 1)

    for i in range(2):
        send_prompts(0, i)
    send_window(0, 1, core == 0)

    acc[...] = jnp.zeros(acc.shape, jnp.float32)

    @pl.when(chip == 0)
    def _():
        kall[:, :, prompt : prompt + 2 * height] = jnp.zeros((half, 2, 2 * height, d), jnp.bfloat16)

    @pl.when(chip == chips - 1)
    def _():
        grecv[...] = jnp.zeros(grecv.shape, jnp.bfloat16)

    lens_local.wait()
    answers = lens.shape[1]
    row = lax.broadcasted_iota(jnp.int32, (answers, answers), 0)
    col = lax.broadcasted_iota(jnp.int32, (answers, answers), 1)
    starts = jnp.sum(
        jnp.where(col < row, jnp.broadcast_to(lst[...], (answers, answers)), 0),
        axis=1, keepdims=True,
    )
    key = lax.broadcasted_iota(jnp.int32, (height, height), 0)
    query = lax.broadcasted_iota(jnp.int32, (height, height), 1)
    tri = key <= query
    for b in range(2):
        base = (2 * chip + b) * height
        pos = base + lax.broadcasted_iota(jnp.int32, (1, height), 1)
        first = jnp.max(jnp.where(starts <= pos, starts, 0), axis=0, keepdims=True)
        bias[b, 0] = jnp.where(key + (base - height) >= first, 0.0, MASKED)
        both = jnp.where(tri, key + base, key + (base - 2 * height))
        bias[b, 1] = jnp.where(both >= first, 0.0, MASKED)
    tri_b[...] = tri.astype(jnp.float32).astype(jnp.bfloat16)

    def prepare(s, j):
        for h in range(group):
            rows = slice(h * height, (h + 1) * height)
            og_t = qog[s, j, 1, :, rows].T
            cots_t[s, j, :, rows] = (wst[s] * og_t.astype(jnp.float32)).astype(jnp.bfloat16)
            qs_t[s, j, :, rows] = qog[s, j, 0, :, rows].T

    w_local.wait()

    @pl.loop(0, half)
    def _(j):
        pltpu.make_async_copy(qog.at[1, j], qog.at[1, j], in_sem.at[j]).wait()
        prepare(1, j)

    for j in range(1, half):
        for i in range(2):
            send_prompts(j, i)
    w_cross.wait_recv()

    @pl.loop(0, half)
    def _(j):
        pltpu.make_async_copy(qog.at[0, j], qog.at[0, j], xq_recv.at[j]).wait()
        prepare(0, j)

    for j in range(1, half):
        for i in range(2):
            send_window(j, i, True)
    pltpu.make_async_copy(pgath.at[0, 0], pgath.at[0, 0], pg_recv.at[0, 0]).wait()

    def assemble(j, i):
        if j > 0 or i > 0:
            pltpu.make_async_copy(pgath.at[j, i], pgath.at[j, i], pg_recv.at[j, i]).wait()
        gathered = pgath[j, i].astype(jnp.float32).reshape(prompt, d)
        kall[j, i, :prompt, :] = gathered.astype(jnp.bfloat16)

    def arrive(j, i, b, leading):
        if leading:
            assemble(j, i)

        @pl.when(chip > 0)
        def _():
            for t in ((0,) if b == 0 else ()) + ((1,) if leading else ()):
                window = kall.at[j, i, block(t)]
                pltpu.make_async_copy(window, window, win_recv.at[j, t, i]).wait()

    def run_unit(j, b, leading):
        s = core if b == 1 else other
        if leading:
            mine = kall.at[j, :, block(2 + core)]
            pltpu.make_async_copy(mine, mine, kv_sem.at[j]).wait()
            theirs = kall.at[j, :, block(2 + other)]
            pltpu.make_async_copy(theirs, theirs, xk_recv.at[j]).wait()
        arrive(j, 0, b, leading)
        late = leading and j == 0
        if not late:
            arrive(j, 1, b, leading)

        near_far = slice(prompt + b * height, prompt + (b + 3) * height)
        tri2 = twice(tri)
        keys = jnp.concatenate([kall[j, 0, :prompt], kall[j, 0, near_far]], axis=0)

        def values():
            return jnp.concatenate([kall[j, 1, :prompt], kall[j, 1, near_far]], axis=0)

        if not late:
            vt[...] = values().T
        held = {}

        def rows_of(pair):
            return slice(pair * 2 * height, (pair + 1) * 2 * height)

        def score(pair):
            scores = dot(keys, qs_t[s, j, :, rows_of(pair)])
            s_p = scores[:at1]
            s_n = scores[at2:at3] + twice(bias[b, 0])
            s_c = jnp.where(tri2, scores[at3:], scores[at1:at2]) + twice(bias[b, 1])
            top = jnp.maximum(
                jnp.maximum(jnp.max(s_p, axis=0, keepdims=True), jnp.max(s_n, axis=0, keepdims=True)),
                jnp.max(s_c, axis=0, keepdims=True),
            )
            held[pair] = s_p, s_n, s_c, top

        def soften(pair):
            rows = rows_of(pair)
            s_p, s_n, s_c, top = held[pair]
            e_p = jnp.exp2((s_p - top) * log_factor)
            e_n = jnp.exp2((s_n - top) * log_factor)
            e_c = jnp.exp2((s_c - top) * log_factor)
            total = (
                jnp.sum(e_p, axis=0, keepdims=True)
                + jnp.sum(e_n, axis=0, keepdims=True)
                + jnp.sum(e_c, axis=0, keepdims=True)
            )
            p_all[s, j, :at1, rows] = e_p.astype(jnp.bfloat16)
            p_all[s, j, at2:at3, rows] = e_n.astype(jnp.bfloat16)
            b_c = e_c.astype(jnp.bfloat16)
            b_d = b_c * twice(tri_b[...])
            p_all[s, j, at1:at2, rows] = b_c - b_d
            p_all[s, j, at3:, rows] = b_d
            held[pair] = 1.0 / total

        def attend(pair):
            rows = rows_of(pair)
            inv = held[pair]
            out_t = (dot(vt[...], p_all[s, j, :, rows]) * inv).astype(jnp.bfloat16)
            cot_t = (cots_t[s, j, :, rows].astype(jnp.float32) * inv).astype(jnp.bfloat16)
            delta = jnp.sum(
                cot_t.astype(jnp.float32) * out_t.astype(jnp.float32), axis=0, keepdims=True
            )
            cots_t[s, j, :, rows] = cot_t
            deltas[s, j, :, rows] = delta
            cots[s, j, rows, :] = cot_t.T
            out = out_t.T
            for h in range(2):
                lanes = slice((2 * pair + h) * d, (2 * pair + h + 1) * d)
                attn[s, j, :, lanes] = out[h * height : (h + 1) * height]
            held[pair] = cot_t, delta

        rows = slice(0, at3 if b == 0 else at2)

        def slope(pair):
            lanes = rows_of(pair)
            cot_t, delta = held[pair]
            slopes = dot(values()[rows], cot_t)
            ds_all[s, j, rows, lanes] = p_all[s, j, rows, lanes] * (slopes - delta).astype(jnp.bfloat16)

        pairs = group // 2
        for step in range(-2, pairs + 2):
            if 0 <= step < pairs:
                soften(step)
            if 0 <= step + 2 < pairs:
                score(step + 2)
            if late and step == 0:
                arrive(j, 1, b, leading)
                vt[...] = values().T
            if 0 <= step - 1 < pairs:
                attend(step - 1)
            if 0 <= step - 2 < pairs:
                slope(step - 2)

        key_terms(j, b, 0, rows)
        key_terms(j, b, 1, rows)
        @pl.when(s == 0)
        def _():
            out_copy(attn, j, at_send, at_recv).start()

    def key_terms(j, b, i, rows):
        s = core if b == 1 else other
        start = max(rows.start, at1)
        window = slice(start + b * height, rows.stop + b * height)
        if i == 0:
            q_rows = jnp.concatenate([qog[s, j, 0, :, h * d : (h + 1) * d] for h in range(group)], axis=0)
            part = dot(ds_all[s, j, rows], q_rows) * factor
        else:
            part = dot(p_all[s, j, rows], cots[s, j])
        if rows.start == 0:
            acc[j, i, :prompt] += part[:at1]
        acc[j, i, window] += part[start - rows.start :]

    def local_rows(b):
        return slice(at3 if b == 0 else at2, at3 + height)

    def local_slope(j, b):
        s = core if b == 1 else other
        rows = local_rows(b)
        values = kall[j, 1, rows.start + b * height : rows.stop + b * height]
        for pair in range(group // 2):
            lanes = slice(pair * 2 * height, (pair + 1) * 2 * height)
            slopes = dot(values, cots_t[s, j, :, lanes])
            ds_all[s, j, rows, lanes] = p_all[s, j, rows, lanes] * (
                slopes - deltas[s, j, :, lanes]
            ).astype(jnp.bfloat16)

    for j in range(half):
        for place, b in enumerate((1, 0) if j == 0 else (0, 1)):
            run_unit(j, b, place == 0)
            if j > 0 and b == 0:
                send_back(j, 0, pl.ds(0, 2))
        send_reduce(j, pl.ds(0, 2))
        if j == 0:
            send_back(j, 0, pl.ds(0, 2))
        send_back(j, 1, pl.ds(0, 2))

    for j in range(half):
        for b in range(2):
            local_slope(j, b)

    @pl.loop(0, 2 * half)
    def _(u):
        s = u // half
        j = lax.rem(u, half)
        b = s * core + (1 - s) * other
        near_far = pl.ds(pl.multiple_of(prompt + b * height, height), 3 * height)
        kt[:, :at1] = kall[j, 0, :prompt].T
        kt[:, at1:] = kall[j, 0, near_far].T
        dq_t = (dot(kt[...], ds_all[s, j]) * factor).astype(jnp.bfloat16)
        for h in range(group):
            rows = slice(h * height, (h + 1) * height)
            dq[s, j, :, rows] = dq_t[:, rows].T

        @pl.when(s == 0)
        def _():
            out_copy(dq, j, dq_send, dq_recv).start()

    for j in range(half):
        for i in range(2):
            for b in range(2):
                key_terms(j, b, i, local_rows(b))
        sibling_copy(j).start()

    for j in range(half):
        sibling_copy(j).wait_recv()

        @pl.when(chip < chips - 1)
        def _():
            back = grecv.at[:, j]
            pltpu.make_async_copy(back, back, gr_recv.at[j]).wait()

        for i, grad in enumerate((akg, avg)):
            mine = acc[j, i, block(2 + core)] + grecv[core, j, i].astype(jnp.float32)
            grad[:, cols(core * half + j, d)] = mine.astype(jnp.bfloat16)
            mine = srecv[j, i] + grecv[other, j, i].astype(jnp.float32)
            grad[:, cols(other * half + j, d)] = mine.astype(jnp.bfloat16)
    for j in range(half):
        terms = precv.at[:, j]
        pltpu.make_async_copy(terms, terms, pr_recv.at[j]).wait()
        for t in range(2):
            lanes = slice((t * half + j) * d, (t * half + j + 1) * d)
            for i, grad in enumerate((pkg, pvg)):
                grad[:, lanes] = jnp.sum(precv[t, j, i].astype(jnp.float32), axis=0)

    w_cross.wait_send()
    for j in range(half):
        sent = pgath.at[j, :, pl.ds(0, n - 1)]
        pltpu.make_async_copy(sent, sent, pg_send.at[j]).wait()
        pltpu.make_async_copy(qog.at[1, j], qog.at[1, j], xq_send.at[j]).wait()
        mine = kall.at[j, :, block(2 + core)]
        pltpu.make_async_copy(mine, mine, xk_send.at[j]).wait()

        @pl.when(chip < chips - 1)
        def _():
            window = kall.at[j, :, pl.ds(prompt, 2 * height)]
            pltpu.make_async_copy(window, window, win_send.at[j]).wait()

        @pl.when(chip > 0)
        def _():
            for t in range(2):
                back_copy(j, t, pl.ds(0, 2)).wait_send()

        sent = psend.at[j, :, pl.ds(0, n - 1)]
        pltpu.make_async_copy(sent, sent, pr_send.at[j]).wait()
        sibling_copy(j).wait_send()
        out_copy(attn, j, at_send, at_recv).wait()
        out_copy(dq, j, dq_send, dq_recv).wait()


def write_out(kv_heads, span, attn, dq, akg, avg, pkg, pvg, *refs):
    outs, (wide_sem, sem) = refs[:6], refs[6:]
    half = kv_heads // 2
    core = lax.rem(lax.axis_index("row"), 2)
    copies = [
        pltpu.make_async_copy(
            v.at[1 + t, j],
            out.at[:, pl.ds(pl.multiple_of((jnp.abs(core - t) * half + j) * span, span), span)],
            wide_sem.at[i, t, j],
        )
        for i, (v, out) in enumerate(((attn, outs[0]), (dq, outs[1])))
        for t in range(2)
        for j in range(half)
    ] + [
        pltpu.make_async_copy(v, out, sem.at[i])
        for i, (v, out) in enumerate(zip((akg, avg, pkg, pvg), outs[2:]))
    ]
    for copy in copies:
        copy.start()
    for copy in copies:
        copy.wait()


def per_device(n, queries, answer_keys, answer_values, prompt_keys, prompt_values, out_grad, weights, lengths):
    height = queries.shape[0]
    d = HEAD_DIM
    columns = answer_keys.shape[1]
    kv_heads = columns // d
    half = kv_heads // 2
    chips = n // 2
    group = queries.shape[1] // columns
    own_prompt = prompt_keys.shape[0]
    keys = own_prompt * n + 3 * height
    held = own_prompt * n + 4 * height
    span = group * d
    answers = lengths.shape[0]
    bf16, f32 = jnp.bfloat16, jnp.float32
    vmem = pl.BlockSpec(memory_space=pltpu.VMEM)
    hbm = pl.BlockSpec(memory_space=pltpu.HBM)
    dma = pltpu.SemaphoreType.DMA
    results = pl.pallas_call(
        functools.partial(kernel, n, kv_heads, group),
        out_shape=(
            pltpu.VMEM((3, half, height, span), bf16),
            pltpu.VMEM((3, half, height, span), bf16),
            pltpu.VMEM(answer_keys.shape, bf16),
            pltpu.VMEM(answer_keys.shape, bf16),
            pltpu.VMEM(prompt_keys.shape, f32),
            pltpu.VMEM(prompt_keys.shape, f32),
        ),
        in_specs=[hbm] * 8,
        out_specs=(vmem,) * 6,
        scratch_shapes=[
            pltpu.VMEM((2, half, 2, height, span), bf16),
            pltpu.VMEM((half, 2, held, d), bf16),
            pltpu.VMEM((d, keys), bf16),
            pltpu.VMEM((d, keys), bf16),
            pltpu.VMEM((half, 2, n, own_prompt, d), bf16),
            pltpu.VMEM((2, 1, height), f32),
            pltpu.VMEM((1, answers), jnp.int32),
            pltpu.VMEM((2, half, d, group * height), bf16),
            pltpu.VMEM((2, half, group * height, d), bf16),
            pltpu.VMEM((2, half, d, group * height), bf16),
            pltpu.VMEM((2, half, keys, group * height), bf16),
            pltpu.VMEM((2, half, keys, group * height), bf16),
            pltpu.VMEM((half, 2, held, d), f32),
            pltpu.VMEM((half, 2, n, own_prompt, d), bf16),
            pltpu.VMEM((2, half, 2, chips, own_prompt, d), bf16),
            pltpu.VMEM((half, 2, 2, height, d), bf16),
            pltpu.VMEM((2, half, 2, height, d), bf16),
            pltpu.VMEM((half, 2, height, d), f32),
            pltpu.VMEM((2, 2, height, height), f32),
            pltpu.VMEM((height, height), bf16),
            pltpu.VMEM((2, half, 1, group * height), f32),
            dma((2,)),
            dma((half,)), dma((half,)), dma((half,)), dma((half,)),
            dma((half, 2, 2)),
            dma((half, 2)),
            *[dma((half,))] * 10,
            dma((half, 2)),
            *[dma((half,))] * 3,
            dma, dma,
            pltpu.SemaphoreType.REGULAR,
        ],
        compiler_params=pltpu.CompilerParams(
            collective_id=0, has_side_effects=True, vmem_limit_bytes=60 * 1024 * 1024
        ),
    )(
        queries, out_grad, answer_keys, answer_values, prompt_keys, prompt_values,
        weights.reshape(1, height), lengths.reshape(1, answers),
    )
    return pl.pallas_call(
        functools.partial(write_out, kv_heads, span),
        out_shape=(
            jax.ShapeDtypeStruct(queries.shape, bf16),
            jax.ShapeDtypeStruct(queries.shape, bf16),
            jax.ShapeDtypeStruct(answer_keys.shape, bf16),
            jax.ShapeDtypeStruct(answer_keys.shape, bf16),
            jax.ShapeDtypeStruct(prompt_keys.shape, f32),
            jax.ShapeDtypeStruct(prompt_keys.shape, f32),
        ),
        in_specs=[vmem] * 6,
        out_specs=(hbm,) * 6,
        scratch_shapes=[dma((2, 2, half)), dma((4,))],
        compiler_params=pltpu.CompilerParams(vmem_limit_bytes=8 * 1024 * 1024),
    )(*results)


def solution(mesh):
    both = ("grp", "row")
    wide = P(both, None)
    return jax.shard_map(
        functools.partial(per_device, mesh.shape["row"]),
        mesh=mesh,
        in_specs=(wide,) * 6 + (P(both), P("grp")),
        out_specs=(wide,) * 6,
        check_vma=False,
    )
```

```python
import functools
import math

import jax
import jax.numpy as jnp
from jax import lax
from jax.experimental import pallas as pl
from jax.experimental.pallas import tpu as pltpu
from jax.sharding import PartitionSpec as P

HEAD_DIM = 128
MASKED = -1e30
MESH = pl.DeviceIdType.MESH


def dot(a, b):
    return jnp.dot(a, b, preferred_element_type=jnp.float32)


def twice(x):
    return jnp.concatenate([x, x], axis=1)


def kernel(
    n, kv_heads, group,
    q_hbm, og_hbm, ak, av, pk, pv, w, lens,
    attn, dq, akg, avg, pkg, pvg,
    qog, kall, vt, kt, pgath, wst, lst, qs_t, cots, cots_t, p_all, ds_all, acc,
    psend, precv, gsend, grecv, srecv, bias, tri_b, deltas, early,
    small_sem, in_sem, kv_sem, xq_recv, xk_recv, win_recv, pg_recv, pr_recv, gr_recv, sr_recv, at_recv, dq_recv,
    xq_send, xk_send, win_send, pg_send, pr_send, gs_send, sr_send, at_send, dq_send, w_recv, w_send, go,
):
    me = lax.axis_index("row")
    height = ak.shape[0]
    d = HEAD_DIM
    span = group * d
    half = kv_heads // 2
    own_prompt = pk.shape[0]
    prompt = own_prompt * n
    factor = d ** (-0.5)
    log_factor = factor * math.log2(math.e)
    chips = n // 2
    core = lax.rem(me, 2)
    other = 1 - core
    chip = me // 2
    sibling = me + 1 - 2 * core
    after = lax.rem(chip + 1, chips)
    before = lax.rem(chip + chips - 1, chips)
    at1, at2, at3 = prompt, prompt + height, prompt + 2 * height

    def remote(src, dst, send, recv, target):
        return pltpu.make_async_remote_copy(
            src_ref=src, dst_ref=dst, send_sem=send, recv_sem=recv,
            device_id={"row": target}, device_id_type=MESH,
        )

    def cols(at, width):
        return pl.ds(pl.multiple_of(at * width, width), width)

    def block(b):
        return pl.ds(pl.multiple_of(prompt + b * height, height), height)

    def in_copies(j):
        head = core * half + j
        return (
            pltpu.make_async_copy(q_hbm.at[:, cols(head, span)], qog.at[1, j, 0], in_sem.at[j]),
            pltpu.make_async_copy(og_hbm.at[:, cols(head, span)], qog.at[1, j, 1], in_sem.at[j]),
        )

    def cross_copies(j):
        head = other * half + j
        return (
            remote(og_hbm.at[:, cols(head, span)], qog.at[0, j, 1], xq_send.at[j], xq_recv.at[j], sibling),
            remote(q_hbm.at[:, cols(head, span)], qog.at[0, j, 0], xq_send.at[j], xq_recv.at[j], sibling),
        )

    def kv_copies(j):
        head = core * half + j
        return [
            pltpu.make_async_copy(src.at[:, cols(head, d)], kall.at[j, i, block(2 + core)], kv_sem.at[j])
            for i, src in enumerate((ak, av))
        ]

    def kv_cross(j):
        head = other * half + j
        return [
            remote(src.at[:, cols(head, d)], kall.at[j, i, block(2 + core)], xk_send.at[j], xk_recv.at[j], sibling)
            for i, src in enumerate((ak, av))
        ]

    def win_copy(j, i, t):
        return remote(
            (ak, av)[i].at[:, pl.ds((t * half + j) * d, d)], kall.at[j, i, block(core)],
            win_send.at[j], win_recv.at[j, core, i], 2 * after + t,
        )

    def prompt_copy(j, k, i):
        target = lax.rem(me + k, n)
        return remote(
            (pk, pv)[i].at[:, cols(lax.rem(target, 2) * half + j, d)], pgath.at[j, i, me],
            pg_send.at[j], pg_recv.at[j, i], target,
        )

    def reduce_copy(j, k, part):
        target = lax.rem(me + k, n)
        return remote(
            psend.at[j, part, target], precv.at[core, j, part, chip], pr_send.at[j], pr_recv.at[j], target
        )

    def send_reduce(j, part):
        for i in range(part.start, part.start + part.size):
            psend[j, i] = acc[j, i, :prompt].reshape(n, own_prompt, d).astype(jnp.bfloat16)

        @pl.loop(1, n)
        def _(k):
            reduce_copy(j, k, part).start()

        pltpu.make_async_copy(psend.at[j, part, me], precv.at[core, j, part, chip], pr_recv.at[j]).start()

    def back_copy(j, t, part):
        return remote(
            gsend.at[j, t, part], grecv.at[core, j, part], gs_send.at[j, t], gr_recv.at[j], 2 * before + t
        )

    def send_back(j, t, part):
        for i in range(part.start, part.start + part.size):
            gsend[j, t, i] = acc[j, i, prompt + t * height : prompt + (t + 1) * height].astype(jnp.bfloat16)

        @pl.when(chip > 0)
        def _():
            back_copy(j, t, part).start()

    def sibling_copy(j):
        return remote(acc.at[j, :, block(2 + other)], srecv.at[j], sr_send.at[j], sr_recv.at[j], sibling)

    def out_copy(ref, j, send, recv):
        return remote(ref.at[0, j], ref.at[2, j], send.at[j], recv.at[j], sibling)

    barrier = pltpu.get_barrier_semaphore()

    def signal(semaphore, target):
        pl.semaphore_signal(semaphore, inc=1, device_id={"row": target}, device_id_type=MESH)

    collector = n - 2

    @pl.when(me < n - 4)
    def _():
        signal(barrier, collector)

    @pl.when(chip > 0)
    def _():
        for t in range(2):
            signal(barrier, 2 * before + t)

    @pl.when(chip < chips - 1)
    def _():
        for t in range(2):
            signal(barrier, 2 * after + t)

    signal(barrier, sibling)

    w_local = pltpu.make_async_copy(w, wst.at[1], small_sem.at[0])
    lens_local = pltpu.make_async_copy(lens, lst, small_sem.at[1])
    own_prompts = [
        pltpu.make_async_copy((pk, pv)[i].at[:, cols(core * half + j, d)], pgath.at[j, i, me], pg_recv.at[j, i])
        for j in range(half)
        for i in range(2)
    ]
    w_local.start()
    lens_local.start()
    for j in range(half):
        for copy in in_copies(j):
            copy.start()
    for j in range(half):
        for copy in kv_copies(j):
            copy.start()
    for copy in own_prompts:
        copy.start()
    @pl.when(me == collector)
    def _():
        pl.semaphore_wait(barrier, n - 1)

        @pl.loop(1, n)
        def _(k):
            signal(go, lax.rem(me + k, n))

    @pl.when(me != collector)
    def _():
        pl.semaphore_wait(
            barrier, 1 + 2 * (chip > 0).astype(jnp.int32) + 2 * (chip < chips - 1).astype(jnp.int32)
        )


    def send_prompts(j, i):
        @pl.loop(1, n)
        def _(k):
            prompt_copy(j, k, i).start()

    def send_window(j, i, condition):
        @pl.when(jnp.logical_and(chip < chips - 1, condition))
        def _():
            for t in range(2):
                win_copy(j, i, t).start()

    w_cross = remote(w, wst.at[0], w_send, w_recv, sibling)
    w_cross.start()
    for i in range(2):
        send_window(0, i, core == 1)
    send_window(0, 0, core == 0)
    for j in range(half):
        for copy in cross_copies(j):
            copy.start()
        for copy in kv_cross(j):
            copy.start()

    @pl.when(me != collector)
    def _():
        pl.semaphore_wait(go, 1)

    for i in range(2):
        send_prompts(0, i)
    send_window(0, 1, core == 0)

    acc[...] = jnp.zeros(acc.shape, jnp.float32)

    @pl.when(chip == 0)
    def _():
        kall[:, :, prompt : prompt + 2 * height] = jnp.zeros((half, 2, 2 * height, d), jnp.bfloat16)

    @pl.when(chip == chips - 1)
    def _():
        grecv[...] = jnp.zeros(grecv.shape, jnp.bfloat16)

    lens_local.wait()
    answers = lens.shape[1]
    row = lax.broadcasted_iota(jnp.int32, (answers, answers), 0)
    col = lax.broadcasted_iota(jnp.int32, (answers, answers), 1)
    starts = jnp.sum(
        jnp.where(col < row, jnp.broadcast_to(lst[...], (answers, answers)), 0),
        axis=1, keepdims=True,
    )
    key = lax.broadcasted_iota(jnp.int32, (height, height), 0)
    query = lax.broadcasted_iota(jnp.int32, (height, height), 1)
    tri = key <= query
    for b in range(2):
        base = (2 * chip + b) * height
        pos = base + lax.broadcasted_iota(jnp.int32, (1, height), 1)
        first = jnp.max(jnp.where(starts <= pos, starts, 0), axis=0, keepdims=True)
        bias[b, 0] = jnp.where(key + (base - height) >= first, 0.0, MASKED)
        both = jnp.where(tri, key + base, key + (base - 2 * height))
        bias[b, 1] = jnp.where(both >= first, 0.0, MASKED)
    tri_b[...] = tri.astype(jnp.float32).astype(jnp.bfloat16)

    def prepare(s, j):
        for h in range(group):
            rows = slice(h * height, (h + 1) * height)
            og_t = qog[s, j, 1, :, rows].T
            cots_t[s, j, :, rows] = (wst[s] * og_t.astype(jnp.float32)).astype(jnp.bfloat16)
            qs_t[s, j, :, rows] = qog[s, j, 0, :, rows].T

    w_local.wait()

    @pl.loop(0, half)
    def _(j):
        pltpu.make_async_copy(qog.at[1, j], qog.at[1, j], in_sem.at[j]).wait()
        prepare(1, j)

    for j in range(1, half):
        for i in range(2):
            send_window(j, i, core == 1)
    w_cross.wait_recv()

    @pl.loop(0, half)
    def _(j):
        pltpu.make_async_copy(qog.at[0, j], qog.at[0, j], xq_recv.at[j]).wait()
        prepare(0, j)


    for j in range(1, half):
        for i in range(2):
            send_prompts(j, i)
    for j in range(1, half):
        for i in range(2):
            send_window(j, i, core == 0)
    def assemble(j, i):
        pltpu.make_async_copy(pgath.at[j, i], pgath.at[j, i], pg_recv.at[j, i]).wait()
        gathered = pgath[j, i].astype(jnp.float32).reshape(prompt, d)
        kall[j, i, :prompt, :] = gathered.astype(jnp.bfloat16)

    def arrive(j, i, b, leading):
        @pl.when(chip > 0)
        def _():
            for t in ((0,) if b == 0 else ()) + ((1,) if leading else ()):
                window = kall.at[j, i, block(t)]
                pltpu.make_async_copy(window, window, win_recv.at[j, t, i]).wait()

    def run_unit(j, b, leading):
        s = core if b == 1 else other
        if leading:
            mine = kall.at[j, :, block(2 + core)]
            pltpu.make_async_copy(mine, mine, kv_sem.at[j]).wait()
            theirs = kall.at[j, :, block(2 + other)]
            pltpu.make_async_copy(theirs, theirs, xk_recv.at[j]).wait()
        arrive(j, 0, b, leading)
        late = leading and j == 0
        if not late:
            arrive(j, 1, b, leading)
            if leading:
                assemble(j, 0)
                assemble(j, 1)

        near_far = slice(prompt + b * height, prompt + (b + 3) * height)
        tri2 = twice(tri)
        def values():
            return jnp.concatenate([kall[j, 1, :prompt], kall[j, 1, near_far]], axis=0)

        if not late:
            vt[...] = values().T
        held = {}
        tops = {}

        def rows_of(pair):
            return slice(pair * 2 * height, (pair + 1) * 2 * height)

        def masked(scores):
            far, near, own = scores[:height], scores[height : 2 * height], scores[2 * height :]
            s_n = near + twice(bias[b, 0])
            s_c = jnp.where(tri2, own, far) + twice(bias[b, 1])
            return s_n, s_c, jnp.maximum(jnp.max(s_n, axis=0, keepdims=True), jnp.max(s_c, axis=0, keepdims=True))

        def score_early(pair):
            s_n, s_c, tops[pair] = masked(dot(kall[j, 0, near_far], qs_t[s, j, :, rows_of(pair)]))
            early[pair, :height] = s_n
            early[pair, height:] = s_c

        def score(pair):
            if late:
                s_p = dot(kall[j, 0, :prompt], qs_t[s, j, :, rows_of(pair)])
                s_n, s_c, top = early[pair, :height], early[pair, height:], tops[pair]
            else:
                keys = jnp.concatenate([kall[j, 0, :prompt], kall[j, 0, near_far]], axis=0)
                scores = dot(keys, qs_t[s, j, :, rows_of(pair)])
                s_p = scores[:at1]
                s_n, s_c, top = masked(scores[at1:])
            held[pair] = s_p, s_n, s_c, jnp.maximum(top, jnp.max(s_p, axis=0, keepdims=True))

        def soften(pair):
            rows = rows_of(pair)
            s_p, s_n, s_c, top = held[pair]
            e_p = jnp.exp2((s_p - top) * log_factor)
            e_n = jnp.exp2((s_n - top) * log_factor)
            e_c = jnp.exp2((s_c - top) * log_factor)
            total = (
                jnp.sum(e_p, axis=0, keepdims=True)
                + jnp.sum(e_n, axis=0, keepdims=True)
                + jnp.sum(e_c, axis=0, keepdims=True)
            )
            p_all[s, j, :at1, rows] = e_p.astype(jnp.bfloat16)
            p_all[s, j, at2:at3, rows] = e_n.astype(jnp.bfloat16)
            b_c = e_c.astype(jnp.bfloat16)
            b_d = b_c * twice(tri_b[...])
            p_all[s, j, at1:at2, rows] = b_c - b_d
            p_all[s, j, at3:, rows] = b_d
            held[pair] = 1.0 / total

        def attend(pair):
            rows = rows_of(pair)
            inv = held[pair]
            out_t = (dot(vt[...], p_all[s, j, :, rows]) * inv).astype(jnp.bfloat16)
            cot_t = (cots_t[s, j, :, rows].astype(jnp.float32) * inv).astype(jnp.bfloat16)
            delta = jnp.sum(
                cot_t.astype(jnp.float32) * out_t.astype(jnp.float32), axis=0, keepdims=True
            )
            cots_t[s, j, :, rows] = cot_t
            deltas[s, j, :, rows] = delta
            cots[s, j, rows, :] = cot_t.T
            out = out_t.T
            for h in range(2):
                lanes = slice((2 * pair + h) * d, (2 * pair + h + 1) * d)
                attn[s, j, :, lanes] = out[h * height : (h + 1) * height]
            held[pair] = cot_t, delta

        rows = slice(0, at3 if b == 0 else at2)

        def slope(pair):
            lanes = rows_of(pair)
            cot_t, delta = held[pair]
            slopes = dot(values()[rows], cot_t)
            ds_all[s, j, rows, lanes] = p_all[s, j, rows, lanes] * (slopes - delta).astype(jnp.bfloat16)

        pairs = group // 2
        if late:
            for pair in range(pairs):
                score_early(pair)
            assemble(j, 0)
        for step in range(-2, pairs + 2):
            if 0 <= step < pairs:
                soften(step)
            if 0 <= step + 2 < pairs:
                score(step + 2)
            if late and step == 1:
                arrive(j, 1, b, leading)
                assemble(j, 1)
                vt[...] = values().T
            if 0 <= step - 1 < pairs:
                attend(step - 1)
            if 0 <= step - 2 < pairs:
                slope(step - 2)

        key_terms(j, b, 0, rows)
        key_terms(j, b, 1, rows)
        @pl.when(s == 0)
        def _():
            out_copy(attn, j, at_send, at_recv).start()

    def key_terms(j, b, i, rows):
        s = core if b == 1 else other
        start = max(rows.start, at1)
        window = slice(start + b * height, rows.stop + b * height)
        if i == 0:
            q_rows = jnp.concatenate([qog[s, j, 0, :, h * d : (h + 1) * d] for h in range(group)], axis=0)
            part = dot(ds_all[s, j, rows], q_rows) * factor
        else:
            part = dot(p_all[s, j, rows], cots[s, j])
        if rows.start == 0:
            acc[j, i, :prompt] += part[:at1]
        acc[j, i, window] += part[start - rows.start :]

    def local_rows(b):
        return slice(at3 if b == 0 else at2, at3 + height)

    def local_slope(j, b):
        s = core if b == 1 else other
        rows = local_rows(b)
        values = kall[j, 1, rows.start + b * height : rows.stop + b * height]
        for pair in range(group // 2):
            lanes = slice(pair * 2 * height, (pair + 1) * 2 * height)
            slopes = dot(values, cots_t[s, j, :, lanes])
            ds_all[s, j, rows, lanes] = p_all[s, j, rows, lanes] * (
                slopes - deltas[s, j, :, lanes]
            ).astype(jnp.bfloat16)

    for j in range(half):
        for place, b in enumerate((1, 0)):
            run_unit(j, b, place == 0)
        send_reduce(j, pl.ds(0, 2))
        if True:
            send_back(j, 0, pl.ds(0, 2))
        send_back(j, 1, pl.ds(0, 2))

    for j in range(half):
        for b in range(2):
            local_slope(j, b)

    @pl.loop(0, 2 * half)
    def _(u):
        s = u // half
        j = lax.rem(u, half)
        b = s * core + (1 - s) * other
        near_far = pl.ds(pl.multiple_of(prompt + b * height, height), 3 * height)
        kt[:, :at1] = kall[j, 0, :prompt].T
        kt[:, at1:] = kall[j, 0, near_far].T
        dq_t = (dot(kt[...], ds_all[s, j]) * factor).astype(jnp.bfloat16)
        for h in range(group):
            rows = slice(h * height, (h + 1) * height)
            dq[s, j, :, rows] = dq_t[:, rows].T

        @pl.when(s == 0)
        def _():
            out_copy(dq, j, dq_send, dq_recv).start()

    for j in range(half):
        for i in range(2):
            for b in range(2):
                key_terms(j, b, i, local_rows(b))
        sibling_copy(j).start()

    for j in range(half):
        sibling_copy(j).wait_recv()

        @pl.when(chip < chips - 1)
        def _():
            back = grecv.at[:, j]
            pltpu.make_async_copy(back, back, gr_recv.at[j]).wait()

        for i, grad in enumerate((akg, avg)):
            mine = acc[j, i, block(2 + core)] + grecv[core, j, i].astype(jnp.float32)
            grad[:, cols(core * half + j, d)] = mine.astype(jnp.bfloat16)
            mine = srecv[j, i] + grecv[other, j, i].astype(jnp.float32)
            grad[:, cols(other * half + j, d)] = mine.astype(jnp.bfloat16)
    for j in range(half):
        terms = precv.at[:, j]
        pltpu.make_async_copy(terms, terms, pr_recv.at[j]).wait()
        for t in range(2):
            lanes = slice((t * half + j) * d, (t * half + j + 1) * d)
            for i, grad in enumerate((pkg, pvg)):
                grad[:, lanes] = jnp.sum(precv[t, j, i].astype(jnp.float32), axis=0)

    w_cross.wait_send()
    for j in range(half):
        sent = pgath.at[j, :, pl.ds(0, n - 1)]
        pltpu.make_async_copy(sent, sent, pg_send.at[j]).wait()
        pltpu.make_async_copy(qog.at[1, j], qog.at[1, j], xq_send.at[j]).wait()
        mine = kall.at[j, :, block(2 + core)]
        pltpu.make_async_copy(mine, mine, xk_send.at[j]).wait()

        @pl.when(chip < chips - 1)
        def _():
            window = kall.at[j, :, pl.ds(prompt, 2 * height)]
            pltpu.make_async_copy(window, window, win_send.at[j]).wait()

        @pl.when(chip > 0)
        def _():
            for t in range(2):
                back_copy(j, t, pl.ds(0, 2)).wait_send()

        sent = psend.at[j, :, pl.ds(0, n - 1)]
        pltpu.make_async_copy(sent, sent, pr_send.at[j]).wait()
        sibling_copy(j).wait_send()
        out_copy(attn, j, at_send, at_recv).wait()
        out_copy(dq, j, dq_send, dq_recv).wait()


def write_out(kv_heads, span, attn, dq, akg, avg, pkg, pvg, *refs):
    outs, (wide_sem, sem) = refs[:6], refs[6:]
    half = kv_heads // 2
    core = lax.rem(lax.axis_index("row"), 2)
    copies = [
        pltpu.make_async_copy(
            v.at[1 + t, j],
            out.at[:, pl.ds(pl.multiple_of((jnp.abs(core - t) * half + j) * span, span), span)],
            wide_sem.at[i, t, j],
        )
        for i, (v, out) in enumerate(((attn, outs[0]), (dq, outs[1])))
        for t in range(2)
        for j in range(half)
    ] + [
        pltpu.make_async_copy(v, out, sem.at[i])
        for i, (v, out) in enumerate(zip((akg, avg, pkg, pvg), outs[2:]))
    ]
    for copy in copies:
        copy.start()
    for copy in copies:
        copy.wait()


def per_device(n, queries, answer_keys, answer_values, prompt_keys, prompt_values, out_grad, weights, lengths):
    height = queries.shape[0]
    d = HEAD_DIM
    columns = answer_keys.shape[1]
    kv_heads = columns // d
    half = kv_heads // 2
    chips = n // 2
    group = queries.shape[1] // columns
    own_prompt = prompt_keys.shape[0]
    keys = own_prompt * n + 3 * height
    held = own_prompt * n + 4 * height
    span = group * d
    answers = lengths.shape[0]
    bf16, f32 = jnp.bfloat16, jnp.float32
    vmem = pl.BlockSpec(memory_space=pltpu.VMEM)
    hbm = pl.BlockSpec(memory_space=pltpu.HBM)
    dma = pltpu.SemaphoreType.DMA
    results = pl.pallas_call(
        functools.partial(kernel, n, kv_heads, group),
        out_shape=(
            pltpu.VMEM((3, half, height, span), bf16),
            pltpu.VMEM((3, half, height, span), bf16),
            pltpu.VMEM(answer_keys.shape, bf16),
            pltpu.VMEM(answer_keys.shape, bf16),
            pltpu.VMEM(prompt_keys.shape, f32),
            pltpu.VMEM(prompt_keys.shape, f32),
        ),
        in_specs=[hbm] * 8,
        out_specs=(vmem,) * 6,
        scratch_shapes=[
            pltpu.VMEM((2, half, 2, height, span), bf16),
            pltpu.VMEM((half, 2, held, d), bf16),
            pltpu.VMEM((d, keys), bf16),
            pltpu.VMEM((d, keys), bf16),
            pltpu.VMEM((half, 2, n, own_prompt, d), bf16),
            pltpu.VMEM((2, 1, height), f32),
            pltpu.VMEM((1, answers), jnp.int32),
            pltpu.VMEM((2, half, d, group * height), bf16),
            pltpu.VMEM((2, half, group * height, d), bf16),
            pltpu.VMEM((2, half, d, group * height), bf16),
            pltpu.VMEM((2, half, keys, group * height), bf16),
            pltpu.VMEM((2, half, keys, group * height), bf16),
            pltpu.VMEM((half, 2, held, d), f32),
            pltpu.VMEM((half, 2, n, own_prompt, d), bf16),
            pltpu.VMEM((2, half, 2, chips, own_prompt, d), bf16),
            pltpu.VMEM((half, 2, 2, height, d), bf16),
            pltpu.VMEM((2, half, 2, height, d), bf16),
            pltpu.VMEM((half, 2, height, d), f32),
            pltpu.VMEM((2, 2, height, height), f32),
            pltpu.VMEM((height, height), bf16),
            pltpu.VMEM((2, half, 1, group * height), f32),
            pltpu.VMEM((group // 2, 2 * height, 2 * height), f32),
            dma((2,)),
            dma((half,)), dma((half,)), dma((half,)), dma((half,)),
            dma((half, 2, 2)),
            dma((half, 2)),
            *[dma((half,))] * 10,
            dma((half, 2)),
            *[dma((half,))] * 3,
            dma, dma,
            pltpu.SemaphoreType.REGULAR,
        ],
        compiler_params=pltpu.CompilerParams(
            collective_id=0, has_side_effects=True, vmem_limit_bytes=60 * 1024 * 1024
        ),
    )(
        queries, out_grad, answer_keys, answer_values, prompt_keys, prompt_values,
        weights.reshape(1, height), lengths.reshape(1, answers),
    )
    return pl.pallas_call(
        functools.partial(write_out, kv_heads, span),
        out_shape=(
            jax.ShapeDtypeStruct(queries.shape, bf16),
            jax.ShapeDtypeStruct(queries.shape, bf16),
            jax.ShapeDtypeStruct(answer_keys.shape, bf16),
            jax.ShapeDtypeStruct(answer_keys.shape, bf16),
            jax.ShapeDtypeStruct(prompt_keys.shape, f32),
            jax.ShapeDtypeStruct(prompt_keys.shape, f32),
        ),
        in_specs=[vmem] * 6,
        out_specs=(hbm,) * 6,
        scratch_shapes=[dma((2, 2, half)), dma((4,))],
        compiler_params=pltpu.CompilerParams(vmem_limit_bytes=8 * 1024 * 1024),
    )(*results)


def solution(mesh):
    both = ("grp", "row")
    wide = P(both, None)
    return jax.shard_map(
        functools.partial(per_device, mesh.shape["row"]),
        mesh=mesh,
        in_specs=(wide,) * 6 + (P(both), P("grp")),
        out_specs=(wide,) * 6,
        check_vma=False,
    )
```

```python
import functools
import math

import jax
import jax.numpy as jnp
from jax import lax
from jax.experimental import pallas as pl
from jax.experimental.pallas import tpu as pltpu
from jax.sharding import PartitionSpec as P

HEAD_DIM = 128
MASKED = -1e30
MESH = pl.DeviceIdType.MESH


def dot(a, b):
    return jnp.dot(a, b, preferred_element_type=jnp.float32)


def twice(x):
    return jnp.concatenate([x, x], axis=1)


def kernel(
    n, kv_heads, group,
    q_hbm, og_hbm, ak, av, pk, pv, w, lens,
    attn, dq, akg, avg, pkg, pvg,
    qog, kall, vt, kt, pgath, wst, lst, qs_t, cots, cots_t, p_all, ds_all, acc,
    psend, precv, gsend, grecv, srecv, bias, tri_b, deltas, early,
    small_sem, in_sem, kv_sem, xq_recv, xk_recv, win_recv, pg_recv, pr_recv, gr_recv, sr_recv, at_recv, dq_recv,
    xq_send, xk_send, win_send, pg_send, pr_send, gs_send, sr_send, at_send, dq_send, w_recv, w_send, go,
):
    me = lax.axis_index("row")
    height = ak.shape[0]
    d = HEAD_DIM
    span = group * d
    half = kv_heads // 2
    own_prompt = pk.shape[0]
    prompt = own_prompt * n
    factor = d ** (-0.5)
    log_factor = factor * math.log2(math.e)
    chips = n // 2
    core = lax.rem(me, 2)
    other = 1 - core
    chip = me // 2
    sibling = me + 1 - 2 * core
    after = lax.rem(chip + 1, chips)
    before = lax.rem(chip + chips - 1, chips)
    at1, at2, at3 = prompt, prompt + height, prompt + 2 * height

    def remote(src, dst, send, recv, target):
        return pltpu.make_async_remote_copy(
            src_ref=src, dst_ref=dst, send_sem=send, recv_sem=recv,
            device_id={"row": target}, device_id_type=MESH,
        )

    def cols(at, width):
        return pl.ds(pl.multiple_of(at * width, width), width)

    def block(b):
        return pl.ds(pl.multiple_of(prompt + b * height, height), height)

    def in_copies(j):
        head = core * half + j
        return (
            pltpu.make_async_copy(q_hbm.at[:, cols(head, span)], qog.at[1, j, 0], in_sem.at[j]),
            pltpu.make_async_copy(og_hbm.at[:, cols(head, span)], qog.at[1, j, 1], in_sem.at[j]),
        )

    def cross_copies(j):
        head = other * half + j
        return (
            remote(og_hbm.at[:, cols(head, span)], qog.at[0, j, 1], xq_send.at[j], xq_recv.at[j], sibling),
            remote(q_hbm.at[:, cols(head, span)], qog.at[0, j, 0], xq_send.at[j], xq_recv.at[j], sibling),
        )

    def kv_copies(j):
        head = core * half + j
        return [
            pltpu.make_async_copy(src.at[:, cols(head, d)], kall.at[j, i, block(2 + core)], kv_sem.at[j])
            for i, src in enumerate((ak, av))
        ]

    def kv_cross(j):
        head = other * half + j
        return [
            remote(src.at[:, cols(head, d)], kall.at[j, i, block(2 + core)], xk_send.at[j], xk_recv.at[j], sibling)
            for i, src in enumerate((ak, av))
        ]

    def win_copy(j, i, t):
        return remote(
            (ak, av)[i].at[:, pl.ds((t * half + j) * d, d)], kall.at[j, i, block(core)],
            win_send.at[j], win_recv.at[j, core, i], 2 * after + t,
        )

    def prompt_copy(j, k, i):
        target = lax.rem(me + k, n)
        return remote(
            (pk, pv)[i].at[:, cols(lax.rem(target, 2) * half + j, d)], pgath.at[j, i, me],
            pg_send.at[j], pg_recv.at[j, i], target,
        )

    def reduce_copy(j, k, part):
        target = lax.rem(me + k, n)
        return remote(
            psend.at[j, part, target], precv.at[core, j, part, chip], pr_send.at[j], pr_recv.at[j], target
        )

    def send_reduce(j, part):
        for i in range(part.start, part.start + part.size):
            psend[j, i] = acc[j, i, :prompt].reshape(n, own_prompt, d).astype(jnp.bfloat16)

        @pl.loop(1, n)
        def _(k):
            reduce_copy(j, k, part).start()

        pltpu.make_async_copy(psend.at[j, part, me], precv.at[core, j, part, chip], pr_recv.at[j]).start()

    def back_copy(j, t, part):
        return remote(
            gsend.at[j, t, part], grecv.at[core, j, part], gs_send.at[j, t], gr_recv.at[j], 2 * before + t
        )

    def send_back(j, t, part):
        for i in range(part.start, part.start + part.size):
            gsend[j, t, i] = acc[j, i, prompt + t * height : prompt + (t + 1) * height].astype(jnp.bfloat16)

        @pl.when(chip > 0)
        def _():
            back_copy(j, t, part).start()

    def sibling_copy(j):
        return remote(acc.at[j, :, block(2 + other)], srecv.at[j], sr_send.at[j], sr_recv.at[j], sibling)

    def out_copy(ref, j, send, recv):
        return remote(ref.at[0, j], ref.at[2, j], send.at[j], recv.at[j], sibling)

    barrier = pltpu.get_barrier_semaphore()

    def signal(semaphore, target):
        pl.semaphore_signal(semaphore, inc=1, device_id={"row": target}, device_id_type=MESH)

    collector = n - 2

    @pl.when(me < n - 4)
    def _():
        signal(barrier, collector)

    @pl.when(chip > 0)
    def _():
        for t in range(2):
            signal(barrier, 2 * before + t)

    @pl.when(chip < chips - 1)
    def _():
        for t in range(2):
            signal(barrier, 2 * after + t)

    signal(barrier, sibling)

    w_local = pltpu.make_async_copy(w, wst.at[1], small_sem.at[0])
    lens_local = pltpu.make_async_copy(lens, lst, small_sem.at[1])
    own_prompts = [
        pltpu.make_async_copy((pk, pv)[i].at[:, cols(core * half + j, d)], pgath.at[j, i, me], pg_recv.at[j, i])
        for j in range(half)
        for i in range(2)
    ]
    w_local.start()
    lens_local.start()
    for j in range(half):
        for copy in in_copies(j):
            copy.start()
    for j in range(half):
        for copy in kv_copies(j):
            copy.start()
    for copy in own_prompts:
        copy.start()
    @pl.when(me == collector)
    def _():
        pl.semaphore_wait(barrier, n - 1)

        @pl.loop(1, n)
        def _(k):
            signal(go, lax.rem(me + k, n))

    @pl.when(me != collector)
    def _():
        pl.semaphore_wait(
            barrier, 1 + 2 * (chip > 0).astype(jnp.int32) + 2 * (chip < chips - 1).astype(jnp.int32)
        )


    def send_prompts(j, i):
        @pl.loop(1, n)
        def _(k):
            prompt_copy(j, k, i).start()

    def send_window(j, i, condition):
        @pl.when(jnp.logical_and(chip < chips - 1, condition))
        def _():
            for t in range(2):
                win_copy(j, i, t).start()

    w_cross = remote(w, wst.at[0], w_send, w_recv, sibling)
    w_cross.start()
    for i in range(2):
        send_window(0, i, core == 1)
    send_window(0, 0, core == 0)
    for j in range(half):
        for copy in cross_copies(j):
            copy.start()
        for copy in kv_cross(j):
            copy.start()

    @pl.when(me != collector)
    def _():
        pl.semaphore_wait(go, 1)

    for i in range(2):
        send_prompts(0, i)
    send_window(0, 1, core == 0)

    for j in range(1, half):
        for i in range(2):
            send_window(j, i, core == 1)
    acc[...] = jnp.zeros(acc.shape, jnp.float32)

    @pl.when(chip == 0)
    def _():
        kall[:, :, prompt : prompt + 2 * height] = jnp.zeros((half, 2, 2 * height, d), jnp.bfloat16)

    @pl.when(chip == chips - 1)
    def _():
        grecv[...] = jnp.zeros(grecv.shape, jnp.bfloat16)

    lens_local.wait()
    answers = lens.shape[1]
    row = lax.broadcasted_iota(jnp.int32, (answers, answers), 0)
    col = lax.broadcasted_iota(jnp.int32, (answers, answers), 1)
    starts = jnp.sum(
        jnp.where(col < row, jnp.broadcast_to(lst[...], (answers, answers)), 0),
        axis=1, keepdims=True,
    )
    key = lax.broadcasted_iota(jnp.int32, (height, height), 0)
    query = lax.broadcasted_iota(jnp.int32, (height, height), 1)
    tri = key <= query
    for b in range(2):
        base = (2 * chip + b) * height
        pos = base + lax.broadcasted_iota(jnp.int32, (1, height), 1)
        first = jnp.max(jnp.where(starts <= pos, starts, 0), axis=0, keepdims=True)
        bias[b, 0] = jnp.where(key + (base - height) >= first, 0.0, MASKED)
        both = jnp.where(tri, key + base, key + (base - 2 * height))
        bias[b, 1] = jnp.where(both >= first, 0.0, MASKED)
    tri_b[...] = tri.astype(jnp.float32).astype(jnp.bfloat16)

    def prepare(s, j):
        for h in range(group):
            rows = slice(h * height, (h + 1) * height)
            og_t = qog[s, j, 1, :, rows].T
            cots_t[s, j, :, rows] = (wst[s] * og_t.astype(jnp.float32)).astype(jnp.bfloat16)
            qs_t[s, j, :, rows] = qog[s, j, 0, :, rows].T

    w_local.wait()

    @pl.loop(0, half)
    def _(j):
        pltpu.make_async_copy(qog.at[1, j], qog.at[1, j], in_sem.at[j]).wait()
        prepare(1, j)

    w_cross.wait_recv()

    @pl.loop(0, half)
    def _(j):
        pltpu.make_async_copy(qog.at[0, j], qog.at[0, j], xq_recv.at[j]).wait()
        prepare(0, j)


    for j in range(1, half):
        for i in range(2):
            send_prompts(j, i)
    for j in range(1, half):
        for i in range(2):
            send_window(j, i, core == 0)
    def assemble(j, i):
        pltpu.make_async_copy(pgath.at[j, i], pgath.at[j, i], pg_recv.at[j, i]).wait()
        gathered = pgath[j, i].astype(jnp.float32).reshape(prompt, d)
        kall[j, i, :prompt, :] = gathered.astype(jnp.bfloat16)

    def arrive(j, i, b, leading):
        @pl.when(chip > 0)
        def _():
            for t in ((0,) if b == 0 else ()) + ((1,) if leading else ()):
                window = kall.at[j, i, block(t)]
                pltpu.make_async_copy(window, window, win_recv.at[j, t, i]).wait()

    def run_unit(j, b, leading):
        s = core if b == 1 else other
        if leading:
            mine = kall.at[j, :, block(2 + core)]
            pltpu.make_async_copy(mine, mine, kv_sem.at[j]).wait()
            theirs = kall.at[j, :, block(2 + other)]
            pltpu.make_async_copy(theirs, theirs, xk_recv.at[j]).wait()
        arrive(j, 0, b, leading)
        late = leading and j == 0
        if not late:
            arrive(j, 1, b, leading)
            if leading:
                assemble(j, 0)
                assemble(j, 1)

        near_far = slice(prompt + b * height, prompt + (b + 3) * height)
        tri2 = twice(tri)
        def values():
            return jnp.concatenate([kall[j, 1, :prompt], kall[j, 1, near_far]], axis=0)

        if not late:
            vt[...] = values().T
        held = {}
        tops = {}

        def rows_of(pair):
            return slice(pair * 2 * height, (pair + 1) * 2 * height)

        def masked(scores):
            far, near, own = scores[:height], scores[height : 2 * height], scores[2 * height :]
            s_n = near + twice(bias[b, 0])
            s_c = jnp.where(tri2, own, far) + twice(bias[b, 1])
            return s_n, s_c, jnp.maximum(jnp.max(s_n, axis=0, keepdims=True), jnp.max(s_c, axis=0, keepdims=True))

        def score_early(pair):
            s_n, s_c, tops[pair] = masked(dot(kall[j, 0, near_far], qs_t[s, j, :, rows_of(pair)]))
            early[pair, :height] = s_n
            early[pair, height:] = s_c

        def score(pair):
            if late:
                s_p = dot(kall[j, 0, :prompt], qs_t[s, j, :, rows_of(pair)])
                s_n, s_c, top = early[pair, :height], early[pair, height:], tops[pair]
            else:
                keys = jnp.concatenate([kall[j, 0, :prompt], kall[j, 0, near_far]], axis=0)
                scores = dot(keys, qs_t[s, j, :, rows_of(pair)])
                s_p = scores[:at1]
                s_n, s_c, top = masked(scores[at1:])
            held[pair] = s_p, s_n, s_c, jnp.maximum(top, jnp.max(s_p, axis=0, keepdims=True))

        def soften(pair):
            rows = rows_of(pair)
            s_p, s_n, s_c, top = held[pair]
            e_p = jnp.exp2((s_p - top) * log_factor)
            e_n = jnp.exp2((s_n - top) * log_factor)
            e_c = jnp.exp2((s_c - top) * log_factor)
            total = (
                jnp.sum(e_p, axis=0, keepdims=True)
                + jnp.sum(e_n, axis=0, keepdims=True)
                + jnp.sum(e_c, axis=0, keepdims=True)
            )
            p_all[s, j, :at1, rows] = e_p.astype(jnp.bfloat16)
            p_all[s, j, at2:at3, rows] = e_n.astype(jnp.bfloat16)
            b_c = e_c.astype(jnp.bfloat16)
            b_d = b_c * twice(tri_b[...])
            p_all[s, j, at1:at2, rows] = b_c - b_d
            p_all[s, j, at3:, rows] = b_d
            held[pair] = 1.0 / total

        def attend(pair):
            rows = rows_of(pair)
            inv = held[pair]
            out_t = (dot(vt[...], p_all[s, j, :, rows]) * inv).astype(jnp.bfloat16)
            cot_t = (cots_t[s, j, :, rows].astype(jnp.float32) * inv).astype(jnp.bfloat16)
            delta = jnp.sum(
                cot_t.astype(jnp.float32) * out_t.astype(jnp.float32), axis=0, keepdims=True
            )
            cots_t[s, j, :, rows] = cot_t
            deltas[s, j, :, rows] = delta
            cots[s, j, rows, :] = cot_t.T
            out = out_t.T
            for h in range(2):
                lanes = slice((2 * pair + h) * d, (2 * pair + h + 1) * d)
                attn[s, j, :, lanes] = out[h * height : (h + 1) * height]
            held[pair] = cot_t, delta

        rows = slice(0, at3 if b == 0 else at2)

        def slope(pair):
            lanes = rows_of(pair)
            cot_t, delta = held[pair]
            slopes = dot(values()[rows], cot_t)
            ds_all[s, j, rows, lanes] = p_all[s, j, rows, lanes] * (slopes - delta).astype(jnp.bfloat16)

        pairs = group // 2
        if late:
            for pair in range(pairs):
                score_early(pair)
            assemble(j, 0)
        for step in range(-2, pairs + 2):
            if 0 <= step < pairs:
                soften(step)
            if 0 <= step + 2 < pairs:
                score(step + 2)
            if late and step == 1:
                arrive(j, 1, b, leading)
                assemble(j, 1)
                vt[...] = values().T
            if 0 <= step - 1 < pairs:
                attend(step - 1)
            if 0 <= step - 2 < pairs:
                slope(step - 2)

        key_terms(j, b, 0, rows)
        key_terms(j, b, 1, rows)
        @pl.when(s == 0)
        def _():
            out_copy(attn, j, at_send, at_recv).start()

    def key_terms(j, b, i, rows):
        s = core if b == 1 else other
        start = max(rows.start, at1)
        window = slice(start + b * height, rows.stop + b * height)
        if i == 0:
            q_rows = jnp.concatenate([qog[s, j, 0, :, h * d : (h + 1) * d] for h in range(group)], axis=0)
            part = dot(ds_all[s, j, rows], q_rows) * factor
        else:
            part = dot(p_all[s, j, rows], cots[s, j])
        if rows.start == 0:
            acc[j, i, :prompt] += part[:at1]
        acc[j, i, window] += part[start - rows.start :]

    def local_rows(b):
        return slice(at3 if b == 0 else at2, at3 + height)

    def local_slope(j, b):
        s = core if b == 1 else other
        rows = local_rows(b)
        values = kall[j, 1, rows.start + b * height : rows.stop + b * height]
        for pair in range(group // 2):
            lanes = slice(pair * 2 * height, (pair + 1) * 2 * height)
            slopes = dot(values, cots_t[s, j, :, lanes])
            ds_all[s, j, rows, lanes] = p_all[s, j, rows, lanes] * (
                slopes - deltas[s, j, :, lanes]
            ).astype(jnp.bfloat16)

    for j in range(half):
        for place, b in enumerate((1, 0)):
            run_unit(j, b, place == 0)
        send_reduce(j, pl.ds(0, 2))
        if True:
            send_back(j, 0, pl.ds(0, 2))
        send_back(j, 1, pl.ds(0, 2))

    for j in range(half):
        for b in range(2):
            local_slope(j, b)

    @pl.loop(0, 2 * half)
    def _(u):
        s = u // half
        j = lax.rem(u, half)
        b = s * core + (1 - s) * other
        near_far = pl.ds(pl.multiple_of(prompt + b * height, height), 3 * height)
        kt[:, :at1] = kall[j, 0, :prompt].T
        kt[:, at1:] = kall[j, 0, near_far].T
        dq_t = (dot(kt[...], ds_all[s, j]) * factor).astype(jnp.bfloat16)
        for h in range(group):
            rows = slice(h * height, (h + 1) * height)
            dq[s, j, :, rows] = dq_t[:, rows].T

        @pl.when(s == 0)
        def _():
            out_copy(dq, j, dq_send, dq_recv).start()

    for j in range(half):
        for i in range(2):
            for b in range(2):
                key_terms(j, b, i, local_rows(b))
        sibling_copy(j).start()

    for j in range(half):
        sibling_copy(j).wait_recv()

        @pl.when(chip < chips - 1)
        def _():
            back = grecv.at[:, j]
            pltpu.make_async_copy(back, back, gr_recv.at[j]).wait()

        for i, grad in enumerate((akg, avg)):
            mine = acc[j, i, block(2 + core)] + grecv[core, j, i].astype(jnp.float32)
            grad[:, cols(core * half + j, d)] = mine.astype(jnp.bfloat16)
            mine = srecv[j, i] + grecv[other, j, i].astype(jnp.float32)
            grad[:, cols(other * half + j, d)] = mine.astype(jnp.bfloat16)
    for j in range(half):
        terms = precv.at[:, j]
        pltpu.make_async_copy(terms, terms, pr_recv.at[j]).wait()
        for t in range(2):
            lanes = slice((t * half + j) * d, (t * half + j + 1) * d)
            for i, grad in enumerate((pkg, pvg)):
                grad[:, lanes] = jnp.sum(precv[t, j, i].astype(jnp.float32), axis=0)

    w_cross.wait_send()
    for j in range(half):
        sent = pgath.at[j, :, pl.ds(0, n - 1)]
        pltpu.make_async_copy(sent, sent, pg_send.at[j]).wait()
        pltpu.make_async_copy(qog.at[1, j], qog.at[1, j], xq_send.at[j]).wait()
        mine = kall.at[j, :, block(2 + core)]
        pltpu.make_async_copy(mine, mine, xk_send.at[j]).wait()

        @pl.when(chip < chips - 1)
        def _():
            window = kall.at[j, :, pl.ds(prompt, 2 * height)]
            pltpu.make_async_copy(window, window, win_send.at[j]).wait()

        @pl.when(chip > 0)
        def _():
            for t in range(2):
                back_copy(j, t, pl.ds(0, 2)).wait_send()

        sent = psend.at[j, :, pl.ds(0, n - 1)]
        pltpu.make_async_copy(sent, sent, pr_send.at[j]).wait()
        sibling_copy(j).wait_send()
        out_copy(attn, j, at_send, at_recv).wait()
        out_copy(dq, j, dq_send, dq_recv).wait()


def write_out(kv_heads, span, attn, dq, akg, avg, pkg, pvg, *refs):
    outs, (wide_sem, sem) = refs[:6], refs[6:]
    half = kv_heads // 2
    core = lax.rem(lax.axis_index("row"), 2)
    copies = [
        pltpu.make_async_copy(
            v.at[1 + t, j],
            out.at[:, pl.ds(pl.multiple_of((jnp.abs(core - t) * half + j) * span, span), span)],
            wide_sem.at[i, t, j],
        )
        for i, (v, out) in enumerate(((attn, outs[0]), (dq, outs[1])))
        for t in range(2)
        for j in range(half)
    ] + [
        pltpu.make_async_copy(v, out, sem.at[i])
        for i, (v, out) in enumerate(zip((akg, avg, pkg, pvg), outs[2:]))
    ]
    for copy in copies:
        copy.start()
    for copy in copies:
        copy.wait()


def per_device(n, queries, answer_keys, answer_values, prompt_keys, prompt_values, out_grad, weights, lengths):
    height = queries.shape[0]
    d = HEAD_DIM
    columns = answer_keys.shape[1]
    kv_heads = columns // d
    half = kv_heads // 2
    chips = n // 2
    group = queries.shape[1] // columns
    own_prompt = prompt_keys.shape[0]
    keys = own_prompt * n + 3 * height
    held = own_prompt * n + 4 * height
    span = group * d
    answers = lengths.shape[0]
    bf16, f32 = jnp.bfloat16, jnp.float32
    vmem = pl.BlockSpec(memory_space=pltpu.VMEM)
    hbm = pl.BlockSpec(memory_space=pltpu.HBM)
    dma = pltpu.SemaphoreType.DMA
    results = pl.pallas_call(
        functools.partial(kernel, n, kv_heads, group),
        out_shape=(
            pltpu.VMEM((3, half, height, span), bf16),
            pltpu.VMEM((3, half, height, span), bf16),
            pltpu.VMEM(answer_keys.shape, bf16),
            pltpu.VMEM(answer_keys.shape, bf16),
            pltpu.VMEM(prompt_keys.shape, f32),
            pltpu.VMEM(prompt_keys.shape, f32),
        ),
        in_specs=[hbm] * 8,
        out_specs=(vmem,) * 6,
        scratch_shapes=[
            pltpu.VMEM((2, half, 2, height, span), bf16),
            pltpu.VMEM((half, 2, held, d), bf16),
            pltpu.VMEM((d, keys), bf16),
            pltpu.VMEM((d, keys), bf16),
            pltpu.VMEM((half, 2, n, own_prompt, d), bf16),
            pltpu.VMEM((2, 1, height), f32),
            pltpu.VMEM((1, answers), jnp.int32),
            pltpu.VMEM((2, half, d, group * height), bf16),
            pltpu.VMEM((2, half, group * height, d), bf16),
            pltpu.VMEM((2, half, d, group * height), bf16),
            pltpu.VMEM((2, half, keys, group * height), bf16),
            pltpu.VMEM((2, half, keys, group * height), bf16),
            pltpu.VMEM((half, 2, held, d), f32),
            pltpu.VMEM((half, 2, n, own_prompt, d), bf16),
            pltpu.VMEM((2, half, 2, chips, own_prompt, d), bf16),
            pltpu.VMEM((half, 2, 2, height, d), bf16),
            pltpu.VMEM((2, half, 2, height, d), bf16),
            pltpu.VMEM((half, 2, height, d), f32),
            pltpu.VMEM((2, 2, height, height), f32),
            pltpu.VMEM((height, height), bf16),
            pltpu.VMEM((2, half, 1, group * height), f32),
            pltpu.VMEM((group // 2, 2 * height, 2 * height), f32),
            dma((2,)),
            dma((half,)), dma((half,)), dma((half,)), dma((half,)),
            dma((half, 2, 2)),
            dma((half, 2)),
            *[dma((half,))] * 10,
            dma((half, 2)),
            *[dma((half,))] * 3,
            dma, dma,
            pltpu.SemaphoreType.REGULAR,
        ],
        compiler_params=pltpu.CompilerParams(
            collective_id=0, has_side_effects=True, vmem_limit_bytes=60 * 1024 * 1024
        ),
    )(
        queries, out_grad, answer_keys, answer_values, prompt_keys, prompt_values,
        weights.reshape(1, height), lengths.reshape(1, answers),
    )
    return pl.pallas_call(
        functools.partial(write_out, kv_heads, span),
        out_shape=(
            jax.ShapeDtypeStruct(queries.shape, bf16),
            jax.ShapeDtypeStruct(queries.shape, bf16),
            jax.ShapeDtypeStruct(answer_keys.shape, bf16),
            jax.ShapeDtypeStruct(answer_keys.shape, bf16),
            jax.ShapeDtypeStruct(prompt_keys.shape, f32),
            jax.ShapeDtypeStruct(prompt_keys.shape, f32),
        ),
        in_specs=[vmem] * 6,
        out_specs=(hbm,) * 6,
        scratch_shapes=[dma((2, 2, half)), dma((4,))],
        compiler_params=pltpu.CompilerParams(vmem_limit_bytes=8 * 1024 * 1024),
    )(*results)


def solution(mesh):
    both = ("grp", "row")
    wide = P(both, None)
    return jax.shard_map(
        functools.partial(per_device, mesh.shape["row"]),
        mesh=mesh,
        in_specs=(wide,) * 6 + (P(both), P("grp")),
        out_specs=(wide,) * 6,
        check_vma=False,
    )
```
